128 devices in a mesh: probe: 32 (over y, z_hi, x), tile: 4 (over z_lo, core).
Axes of the slice: x: 4, y: 4, z: 4 (z_hi: 2, z_lo: 2; z = z_hi * 2 + z_lo), core: 2. Of those that a mesh axis runs over, the one named last changes fastest.
Arguments:
- transmission: bfloat16 [2, 2, 2048, 1024], P(None, None, 'tile', 'probe'), may hold values from -4.1875 to 4.1875
- illumination: bfloat16 [2, 512, 512], replicated, may hold values from -3 to 3
- intensities: float32 [64, 512, 512], P('probe'), may hold values from 0 to 1
- scan_positions: int32 [64, 2], P('probe'), may hold values from 0 to 512, as said below
- tile_owner: int32 [64], P('probe'), may hold values from 0 to 3, as said below
Outputs:
- gradient: float32 [2, 2, 2048, 1024], P(None, None, 'tile', 'probe')
- probe_losses: float32 [64], P('probe')
The draws below stay inside these ranges and needn't reach their ends.
Inputs may be any that keep to these rules, and one draw needn't show every extreme that they name: `tile_owner`: of the 2 scan positions held by one device along probe, no two have the same owner. scan_positions[k, 0] counts rows from row tile_owner[k] * 512 - 128 of the object and scan_positions[k, 1] columns from its first column; the 512 x 512 window of every probe lies inside the object and inside its owner's rows widened by 128 on each side.
All inputs are finite; a program needn't handle non-finite values.
Results may differ from the reference program's by a relative error of at most 0.012.
Values may be sent and summed in bfloat16 or wider, within the bound.
No kernel may reach another device: no remote copies, remote signals or barrier semaphores. Data moves between devices by JAX's collectives and lax.ppermute only.
A program may use at most 128 MiB of HBM per device.

```python
import math
import jax
import jax.numpy as jnp
from jax import lax

SLICES = 2
FRAME = 512
BORDER = 128
TILE_ROWS = 512
OBJ_COLS = 1024
PR_DEV = 2
CAP = 1
PROBES = 64
OBJ_ROWS = 2048
N_TILE = 4


def owners_and_places(key):
    base_key = jax.random.fold_in(key, 11)
    subkeys = jax.random.split(base_key, 5)
    shards = PROBES // PR_DEV
    leading = jax.random.randint(subkeys[0], (shards, 1), 0, N_TILE)
    others = (leading + 1 + jax.random.randint(subkeys[1], (shards, PR_DEV - CAP), 0, N_TILE - 1)) % N_TILE
    owners = jnp.concatenate([jnp.broadcast_to(leading, (shards, CAP)), others], axis=1)
    scores = jax.random.randint(subkeys[2], (shards, PR_DEV), 0, 1 << 20) * PR_DEV + jnp.arange(PR_DEV)
    ranking = jnp.argsort(scores, axis=1)
    owners = jnp.take_along_axis(owners, ranking, axis=1).reshape(PROBES)
    local_rows = jax.random.randint(subkeys[3], (PROBES,), 0, TILE_ROWS + 2 * BORDER - FRAME + 1)
    global_rows = jnp.clip(owners * TILE_ROWS - BORDER + local_rows, 0, OBJ_ROWS - FRAME)
    local_rows = global_rows - owners * TILE_ROWS + BORDER
    columns = jax.random.randint(subkeys[4], (PROBES,), 0, OBJ_COLS - FRAME + 1)
    places = jnp.stack([local_rows, columns], axis=1)
    return (owners.astype(jnp.int32), places.astype(jnp.int32))


def draw_tile_owner(key, part):
    return owners_and_places(key)[0]


def draw_scan_positions(key, part):
    return owners_and_places(key)[1]


def block_scale(own_key, dims, cuts, least, largest):
    def one(dim, blocks):
        heights = jax.random.uniform(jax.random.fold_in(jax.random.fold_in(own_key, 6), dim), (blocks,), jnp.float32, least / len(cuts), largest / len(cuts))
        return jnp.repeat(jnp.exp(heights), dims[dim] // blocks).reshape((-1,) + (1,) * (len(dims) - dim - 1))

    factor_of = one(*cuts[0])
    for cut in cuts[1:]:
        factor_of = factor_of * one(*cut)
    return factor_of


def gaussian(own_key, dims, deviation, limit, pieces=(), kind=jnp.bfloat16):
    factor_of = block_scale(own_key, dims, pieces, -0.22, 0.18) if pieces else 1.0
    drawn = jax.random.normal(own_key, dims, jnp.float32) * deviation * factor_of
    return jnp.minimum(jnp.maximum(drawn, -limit), limit).astype(kind)


def setup_inputs(seed: int = 0) -> dict:
    arg_keys = jax.random.split(jax.random.key(seed), 6)
    transmission = gaussian(arg_keys[0], (SLICES, 2, OBJ_ROWS, OBJ_COLS), 0.7, 4.1875, ((2, 4), (3, 32)))
    illumination = gaussian(arg_keys[1], (2, FRAME, FRAME), 0.5, 3.0)
    intensities = jnp.clip(1.0 * jax.random.uniform(arg_keys[2], (PROBES, FRAME, FRAME), jnp.float32) ** block_scale(arg_keys[2], (PROBES, FRAME, FRAME), ((0, 32),), -0.2, 0.2), 0.0, 1.0)
    scan_positions = draw_scan_positions(jax.random.fold_in(arg_keys[5], 71), 0)
    tile_owner = draw_tile_owner(jax.random.fold_in(arg_keys[5], 71), 0)
    return {"transmission": transmission, "illumination": illumination, "intensities": intensities, "scan_positions": scan_positions, "tile_owner": tile_owner}


fresnel = 0.25

def build_tables(frame_size):
    indices = jnp.arange(frame_size, dtype=jnp.int32)
    product = indices[:, None] * indices[None, :] % frame_size
    angle = -2.0 * math.pi * product.astype(jnp.float32) / frame_size
    norming = 1.0 / math.sqrt(frame_size)
    dft_re = jnp.cos(angle) * norming
    dft_im = jnp.sin(angle) * norming
    freq = jnp.where(indices < frame_size // 2, indices, indices - frame_size).astype(jnp.float32)
    phase = -math.pi * fresnel * freq * freq / frame_size
    kernel_re = jnp.cos(phase)[:, None]
    kernel_im = jnp.sin(phase)[:, None]
    scaled_re = kernel_re * dft_re - kernel_im * dft_im
    scaled_im = kernel_re * dft_im + kernel_im * dft_re
    high = lax.Precision.HIGHEST
    prop_re = jnp.dot(dft_re, scaled_re, precision=high) + jnp.dot(dft_im, scaled_im, precision=high)
    prop_im = jnp.dot(dft_re, scaled_im, precision=high) - jnp.dot(dft_im, scaled_re, precision=high)
    wave_re = dft_re.astype(jnp.bfloat16)
    wave_im = dft_im.astype(jnp.bfloat16)
    qmat_re = prop_re.astype(jnp.bfloat16)
    qmat_im = prop_im.astype(jnp.bfloat16)
    prop_tables = (qmat_re, qmat_im, qmat_re.T, qmat_im.T)
    prop_adjoint = (qmat_re.T, -qmat_im.T, qmat_re, -qmat_im)
    far_tables = (wave_re, wave_im, wave_re, wave_im)
    far_adjoint = (wave_re, -wave_im, wave_re, -wave_im)
    return (prop_tables, prop_adjoint, far_tables, far_adjoint)

def complex_dot(left_re, left_im, right_re, right_im):
    real_part = jnp.dot(left_re, right_re, preferred_element_type=jnp.float32) - jnp.dot(left_im, right_im, preferred_element_type=jnp.float32)
    imag_part = jnp.dot(left_re, right_im, preferred_element_type=jnp.float32) + jnp.dot(left_im, right_re, preferred_element_type=jnp.float32)
    return (real_part, imag_part)

def transform(field_re, field_im, table):
    left_re, left_im, right_re, right_im = table
    inner_re, inner_im = complex_dot(field_re.astype(jnp.bfloat16), field_im.astype(jnp.bfloat16), right_re, right_im)
    return complex_dot(left_re, left_im, inner_re.astype(jnp.bfloat16), inner_im.astype(jnp.bfloat16))

def probe_pass(patch, measured, illumination, tables):
    prop_tables, prop_adjoint, far_tables, far_adjoint = tables
    slice_count = patch.shape[0]
    wave_re = illumination[0].astype(jnp.float32)
    wave_im = illumination[1].astype(jnp.float32)
    inputs = []
    for slice_index in range(slice_count):
        inputs.append((wave_re, wave_im))
        layer_re = patch[slice_index, 0].astype(jnp.float32)
        layer_im = patch[slice_index, 1].astype(jnp.float32)
        exit_re = wave_re * layer_re - wave_im * layer_im
        exit_im = wave_re * layer_im + wave_im * layer_re
        if slice_index < slice_count - 1:
            wave_re, wave_im = transform(exit_re, exit_im, prop_tables)
        else:
            far_re, far_im = transform(exit_re, exit_im, far_tables)
    misfit = far_re * far_re + far_im * far_im - measured
    loss_value = jnp.mean(misfit * misfit)
    back_re, back_im = transform(misfit * far_re, misfit * far_im, far_adjoint)
    grad_list = [None] * slice_count
    for slice_index in range(slice_count - 1, -1, -1):
        wave_re, wave_im = inputs[slice_index]
        grad_re = wave_re * back_re + wave_im * back_im
        grad_im = wave_re * back_im - wave_im * back_re
        grad_list[slice_index] = jnp.stack([grad_re, grad_im])
        if slice_index > 0:
            layer_re = patch[slice_index, 0].astype(jnp.float32)
            layer_im = patch[slice_index, 1].astype(jnp.float32)
            carry_re = layer_re * back_re + layer_im * back_im
            carry_im = layer_re * back_im - layer_im * back_re
            back_re, back_im = transform(carry_re, carry_im, prop_adjoint)
    return (jnp.stack(grad_list), loss_value)

def reference(transmission, illumination, intensities, scan_positions, tile_owner):
    tables = build_tables(FRAME)
    zero_index = jnp.zeros((), jnp.int32)
    initial = jnp.zeros((SLICES, 2, OBJ_ROWS, OBJ_COLS), jnp.float32)

    def visit(summed, item):
        measured, position, owner = item
        row_start = (owner * TILE_ROWS - BORDER + position[0]).astype(jnp.int32)
        col_start = position[1].astype(jnp.int32)
        starts = (zero_index, zero_index, row_start, col_start)
        patch = lax.dynamic_slice(transmission, starts, (SLICES, 2, FRAME, FRAME))
        patch_grad, loss_value = probe_pass(patch, measured, illumination, tables)
        current = lax.dynamic_slice(summed, starts, (SLICES, 2, FRAME, FRAME))
        summed = lax.dynamic_update_slice(summed, current + patch_grad, starts)
        return (summed, loss_value)
    gradient, probe_losses = lax.scan(visit, initial, (intensities, scan_positions, tile_owner))
    return (gradient, probe_losses)
```

```python
import math

import jax
import jax.numpy as jnp
import numpy as np
from jax import lax
from jax.sharding import PartitionSpec as P

FRAME = 512
BORDER = 128
TILE_ROWS = 512
FRESNEL = 0.25
ALL = ("probe", "tile")
BF = jnp.bfloat16
F32 = jnp.float32


def natural(order):
    return order // 256 * 256 + order % 8 * 32 + order // 8 % 32


def build_tables():
    n = FRAME
    index = np.arange(n)
    angle = (np.float32(-2.0 * math.pi) * (np.outer(index, index) % n).astype(np.float32) / np.float32(n)).astype(np.float32)
    norm = np.float32(1.0 / math.sqrt(n))
    wave_re, wave_im = np.cos(angle) * norm, np.sin(angle) * norm
    freq = np.where(index < n // 2, index, index - n).astype(np.float32)
    phase = (np.float32(-math.pi * FRESNEL) * freq * freq / np.float32(n)).astype(np.float32)
    kre, kim = np.cos(phase)[:, None], np.sin(phase)[:, None]
    sre, sim = kre * wave_re - kim * wave_im, kre * wave_im + kim * wave_re
    prop_re = wave_re @ sre + wave_im @ sim
    prop_im = wave_re @ sim - wave_im @ sre
    perm = natural(index)
    bf = jnp.bfloat16
    far = (wave_re[perm].astype(bf), wave_im[perm].astype(bf))
    prop = (prop_re[perm][:, perm].astype(bf), prop_im[perm][:, perm].astype(bf))
    return far, prop


def dot(left, right, dims):
    return lax.dot_general(left, right, (dims, ((), ())), preferred_element_type=F32)


def cdot(left, right, dims, conj_left=False, conj_right=False):
    lre, lim = left
    rre, rim = right
    ii = dot(lim, rim, dims)
    rr = dot(lre, rre, dims)
    ri = dot(lre, rim, dims)
    ir = dot(lim, rre, dims)
    re = rr + ii if conj_left != conj_right else rr - ii
    if conj_left:
        ir = -ir
    if conj_right:
        ri = -ri
    return re, ri + ir


def rounded(pair):
    return tuple(v.astype(BF) for v in pair)


NN = ((1,), (0,))
TN = ((0,), (0,))
NT = ((1,), (1,))


def body(transmission, illumination, intensities, scan_positions, tile_owner):
    far_np, prop_np = build_tables()
    far = tuple(jnp.asarray(v) for v in far_np)
    prop = tuple(jnp.asarray(v) for v in prop_np)
    device = lax.axis_index("probe") * 4 + lax.axis_index("tile")
    core = lax.axis_index("tile") % 2
    which = lax.axis_index("tile") // 2
    my_col = device // 4
    my_quarter = device % 4
    order = jnp.arange(FRAME, dtype=jnp.int32)
    residue = natural(order)

    row0 = tile_owner * TILE_ROWS - BORDER + scan_positions[:, 0]
    col0 = scan_positions[:, 1]
    info = jnp.stack([row0 // 32, row0 % 32, col0 // 32, col0 % 32], axis=1).reshape(8).astype(BF)
    place = (residue[None, :] == order[:, None]).astype(BF)
    block = dot(transmission.reshape(4, 512, 32), place, ((1,), (0,))).astype(BF)
    block = block.reshape(4, 32, 4, 128).transpose(1, 2, 0, 3).reshape(128, 4, 128)
    info = jnp.broadcast_to(jnp.pad(info, (0, 120)), (128, 4, 128))
    got = lax.all_to_all(jnp.concatenate([block, info], axis=1), ALL, 0, 0, tiled=True)
    told = got[::4, 4, :8].astype(jnp.int32).reshape(64, 4)
    rows0 = told[:, 0] * 32 + told[:, 1]
    cols0 = told[:, 2] * 32 + told[:, 3]

    cand = got[:, :4].reshape(2, 16, 4, 4, 128).transpose(0, 2, 3, 1, 4)
    column = jnp.arange(16, dtype=jnp.int32) * 32 + my_col
    row = natural(my_quarter * 128 + jnp.arange(128, dtype=jnp.int32))
    half = (column[None, :] < cols0[:, None]).astype(jnp.int32)
    tile = rows0[:, None] // 512 + (row[None, :] < rows0[:, None] % 512)
    pick = tile[:, None, :] + 4 * half[:, :, None]
    sent = jnp.zeros((64, 4, 16, 128), BF)
    for a in range(2):
        for b in range(4):
            sent = jnp.where((pick == 4 * a + b)[:, None], cand[a, b][None], sent)
    sent = sent.reshape(64, 4, 2, 8, 128).transpose(0, 2, 1, 3, 4).reshape(128, 32, 128)
    mine = lax.all_to_all(sent, ALL, 0, 0, tiled=True)
    mine = mine.reshape(32, 4, 4, 8, 128).transpose(2, 0, 3, 1, 4).reshape(4, 256, 512)
    swap = [(0, 1), (1, 0), (2, 3), (3, 2)]
    other = lax.ppermute(mine, "tile", swap)
    first = core == 0
    patch = jnp.concatenate([jnp.where(first, mine, other), jnp.where(first, other, mine)], axis=1)

    my_row0 = lax.dynamic_index_in_dim(row0, which, 0, False)
    my_col0 = lax.dynamic_index_in_dim(col0, which, 0, False)
    roll_cols = ((residue[:, None] - my_col0) % FRAME == order[None, :]).astype(BF)
    roll_rows = ((residue[None, :] - my_row0) % FRAME == order[:, None]).astype(BF)
    wave = []
    for v in (illumination[0], illumination[1]):
        turned = dot(roll_cols, v, NT).astype(BF)
        wave.append(dot(turned, roll_rows, NN))
    layer = patch.astype(F32)
    exit0 = (wave[0] * layer[0] - wave[1] * layer[1], wave[0] * layer[1] + wave[1] * layer[0])
    inner = rounded(cdot(rounded(exit0), prop, NN))
    mid = cdot(prop, inner, NN)
    exit1 = (mid[0] * layer[2] - mid[1] * layer[3], mid[0] * layer[3] + mid[1] * layer[2])
    inner = rounded(cdot(rounded(exit1), far, NN))
    psi = cdot(inner, far, TN)
    measured = lax.dynamic_index_in_dim(intensities, which, 0, False)
    misfit = psi[0] * psi[0] + psi[1] * psi[1] - measured
    loss = jnp.mean(misfit * misfit)
    inner = rounded(cdot(far, rounded((misfit * psi[0], misfit * psi[1])), NT, conj_left=True))
    back = cdot(inner, far, NT, conj_right=True)
    grad1 = (mid[0] * back[0] + mid[1] * back[1], mid[0] * back[1] - mid[1] * back[0])
    carry = (layer[2] * back[0] + layer[3] * back[1], layer[2] * back[1] - layer[3] * back[0])
    inner = rounded(cdot(rounded(carry), prop, NN, conj_right=True))
    back = cdot(prop, inner, NN, conj_left=True)
    grad0 = (wave[0] * back[0] + wave[1] * back[1], wave[0] * back[1] - wave[1] * back[0])

    grad = jnp.stack([v.astype(BF) for v in grad0 + grad1])
    grad = lax.dynamic_slice_in_dim(grad, core * 256, 256, axis=1)
    grad = grad.reshape(4, 32, 8, 4, 128).transpose(1, 3, 0, 2, 4).reshape(128, 32, 128)
    back_home = lax.all_to_all(grad, ALL, 0, 0, tiled=True)
    parts = back_home.reshape(64, 2, 4, 8, 128).transpose(0, 2, 1, 3, 4).reshape(64, 4, 16, 128).astype(F32)
    sums = []
    for a in range(2):
        for b in range(4):
            sums.append(jnp.sum(jnp.where((pick == 4 * a + b)[:, None], parts, 0.0), axis=0))
    sums = jnp.stack(sums).reshape(2, 4, 4, 16, 128).transpose(0, 3, 1, 2, 4).reshape(128, 4, 128)
    final = lax.all_to_all(sums.astype(BF), ALL, 0, 0, tiled=True)
    final = final.reshape(32, 4, 4, 128).transpose(2, 0, 1, 3).reshape(4, 32, 512)
    gradient = lax.dot_general(place, final, (((1,), (2,)), ((), ())), preferred_element_type=F32)
    gradient = gradient.transpose(1, 0, 2).reshape(2, 2, 512, 32)

    loss_other = lax.ppermute(loss[None], "tile", [(0, 2), (1, 3), (2, 0), (3, 1)])
    pair = jnp.concatenate([loss[None], loss_other])
    probe_losses = jnp.where(which == 0, pair, pair[::-1])
    return gradient, probe_losses


def solution(mesh):
    return jax.shard_map(
        body,
        mesh=mesh,
        in_specs=(
            P(None, None, "tile", "probe"),
            P(),
            P("probe", None, None),
            P("probe", None),
            P("probe"),
        ),
        out_specs=(P(None, None, "tile", "probe"), P("probe")),
        check_vma=False,
    )
```

```python
import math

import jax
import jax.numpy as jnp
import numpy as np
from jax import lax
from jax.experimental import pallas as pl
from jax.experimental.pallas import tpu as pltpu
from jax.sharding import Mesh
from jax.sharding import PartitionSpec as P

FRAME = 512
BORDER = 128
TILE_ROWS = 512
FRESNEL = 0.25
PROBE = ("half", "col")
CHIPS = ("half", "col", "zl")
ALL = ("half", "col", "zl", "core")
SHARERS = ("half", "zl", "core")
BF = jnp.bfloat16
F32 = jnp.float32


def natural(order):
    return order % 16 * 32 + order // 16


def build_tables():
    n = FRAME
    index = np.arange(n)
    angle = (np.float32(-2.0 * math.pi) * (np.outer(index, index) % n).astype(np.float32) / np.float32(n)).astype(np.float32)
    norm = np.float32(1.0 / math.sqrt(n))
    wave_re, wave_im = np.cos(angle) * norm, np.sin(angle) * norm
    freq = np.where(index < n // 2, index, index - n).astype(np.float32)
    phase = (np.float32(-math.pi * FRESNEL) * freq * freq / np.float32(n)).astype(np.float32)
    kre, kim = np.cos(phase)[:, None], np.sin(phase)[:, None]
    sre, sim = kre * wave_re - kim * wave_im, kre * wave_im + kim * wave_re
    prop_re = wave_re @ sre + wave_im @ sim
    prop_im = wave_re @ sim - wave_im @ sre
    perm = natural(index)
    bf = jnp.bfloat16
    far = (wave_re[perm].astype(bf), wave_im[perm].astype(bf))
    prop = (prop_re[perm][:, perm].astype(bf), prop_im[perm][:, perm].astype(bf))
    return far, prop


def right_form(re, im):
    re, im = jnp.asarray(re), jnp.asarray(im)
    return jnp.concatenate([jnp.concatenate([re, im], 1), jnp.concatenate([-im, re], 1)], 0)


def dot(left, right, dims):
    return lax.dot_general(left, right, (dims, ((), ())), preferred_element_type=F32)


NN = ((1,), (0,))
NT = ((1,), (1,))


def probe_kernel(
    core_ref, own, other, wave, measured_hbm, bq_hbm, aq_hbm, bw_hbm, aw_hbm, out, loss,
    y, inner, x1, field, turn, measured, bq, aq, bw, aw, sems,
):
    copies = [
        pltpu.make_async_copy(src, dst, sems.at[n])
        for n, (src, dst) in enumerate(
            ((bq_hbm, bq), (aq_hbm, aq), (bw_hbm, bw), (aw_hbm, aw), (measured_hbm, measured))
        )
    ]
    for copy in copies:
        copy.start()
    core = core_ref[0]
    first = core == 0
    here = pl.multiple_of(core * 256, 256)

    def layer(i, z, c, plane):
        mine, rest = own[i, z, c, plane].astype(F32), other[i, z, c, plane].astype(F32)
        return jnp.concatenate([jnp.where(first, mine, rest), jnp.where(first, rest, mine)], axis=0)

    def block_rows(i):
        return pl.ds(pl.multiple_of(i * 16, 16), 16), pl.ds(pl.multiple_of(512 + i * 16, 16), 16)

    def product(plane, get, conj):
        def step(i, _):
            rows, _ = block_rows(i)
            for z in range(2):
                for c in range(2):
                    at = 256 * c + 128 * z
                    ore, oim = layer(i, z, c, plane), layer(i, z, c, plane + 1)
                    vre, vim = get(i, slice(at, at + 128))
                    if conj:
                        re, im = ore * vre + oim * vim, ore * vim - oim * vre
                    else:
                        re, im = ore * vre - oim * vim, ore * vim + oim * vre
                    y[rows, at : at + 128] = re.astype(BF)
                    y[rows, 512 + at : 640 + at] = im.astype(BF)
            return 0

        lax.fori_loop(0, 32, step, 0, unroll=2)

    def from_wave(i, lanes):
        rows, _ = block_rows(i)
        return wave[0, rows, lanes].astype(F32), wave[1, rows, lanes].astype(F32)

    def from_ref(ref):
        def get(i, lanes):
            rows, rows_im = block_rows(i)
            return ref[rows, lanes], ref[rows_im, lanes]

        return get

    def right(table):
        for n in range(4):
            got = jnp.dot(y[...], table[:, n * 256 : n * 256 + 256], preferred_element_type=F32)
            inner[n // 2 * 512 : n // 2 * 512 + 512, n % 2 * 256 : n % 2 * 256 + 256] = got.astype(BF)

    def left(table, dst):
        for n in range(2):
            dst[:, n * 256 : n * 256 + 256] = jnp.dot(
                table[...], inner[:, n * 256 : n * 256 + 256], preferred_element_type=F32
            )

    def hand_out(plane):
        for o in range(4):
            for j in range(16):
                for part in range(2):
                    rows = pl.ds(part * 512 + 128 * o + j, 8, stride=16)
                    for z in range(2):
                        out[o // 2, j, o % 2, z, plane + part] = turn[z, rows, :].astype(BF)

    product(0, from_wave, False)
    copies[0].wait()
    right(bq)
    copies[1].wait()
    left(aq, x1)
    product(2, from_ref(x1), False)
    copies[2].wait()
    right(bw)
    copies[3].wait()
    left(aw, field)
    copies[4].wait()

    def compare(i, total):
        rows, rows_im = block_rows(i)
        re, im = field[rows, :], field[rows_im, :]
        misfit = re * re + im * im - measured[rows, :]
        y[rows, 0:512] = (misfit * re).astype(BF)
        y[rows, 512:1024] = (misfit * im).astype(BF)
        return total + misfit * misfit

    total = lax.fori_loop(0, 32, compare, jnp.zeros((16, 512), F32))
    loss[...] = jnp.full((8, 128), jnp.sum(total) * (1.0 / (FRAME * FRAME)), F32)
    right(aw)
    left(bw, field)
    product(2, from_ref(field), True)

    def gradient1(i, _):
        rows, rows_im = block_rows(i)
        for z in range(2):
            lanes = pl.ds(pl.multiple_of(here + z * 128, 128), 128)
            bre, bim = field[rows, lanes], field[rows_im, lanes]
            xre, xim = x1[rows, lanes], x1[rows_im, lanes]
            turn[z, rows, :] = xre * bre + xim * bim
            turn[z, rows_im, :] = xre * bim - xim * bre
        return 0

    lax.fori_loop(0, 32, gradient1, 0, unroll=2)
    hand_out(2)
    for part in range(2):
        cols = pl.ds(pl.multiple_of(here + part * 512, 256), 256)
        got = jnp.dot(y[...], aq[:, cols], preferred_element_type=F32)
        inner[part * 512 : part * 512 + 512, 0:256] = got.astype(BF)
    field[:, 0:256] = jnp.dot(bq[...], inner[:, 0:256], preferred_element_type=F32)

    def gradient0(i, _):
        rows, rows_im = block_rows(i)
        for z in range(2):
            bre, bim = field[rows, z * 128 : z * 128 + 128], field[rows_im, z * 128 : z * 128 + 128]
            xre, xim = from_wave(i, pl.ds(pl.multiple_of(here + z * 128, 128), 128))
            turn[z, rows, :] = xre * bre + xim * bim
            turn[z, rows_im, :] = xre * bim - xim * bre
        return 0

    lax.fori_loop(0, 32, gradient0, 0, unroll=2)
    hand_out(0)


VM = pl.BlockSpec(memory_space=pltpu.VMEM)
SM = pl.BlockSpec(memory_space=pltpu.SMEM)
ANY = pl.BlockSpec(memory_space=pl.ANY)
PARAMS = pltpu.CompilerParams(vmem_limit_bytes=56 * 2**20)


def probe_step(core, own, other, wave, measured, tables):
    return pl.pallas_call(
        probe_kernel,
        out_shape=(
            jax.ShapeDtypeStruct((2, 16, 2, 2, 4, 8, 128), BF),
            jax.ShapeDtypeStruct((8, 128), F32),
        ),
        in_specs=[SM, VM, VM, VM] + [ANY] * 5,
        out_specs=(VM, VM),
        scratch_shapes=[
            pltpu.VMEM((512, 1024), BF),
            pltpu.VMEM((1024, 512), BF),
            pltpu.VMEM((1024, 512), F32),
            pltpu.VMEM((1024, 512), F32),
            pltpu.VMEM((2, 1024, 128), F32),
            pltpu.VMEM((512, 512), F32),
        ]
        + [pltpu.VMEM((1024, 1024), BF)] * 4
        + [pltpu.SemaphoreType.DMA((5,))],
        compiler_params=PARAMS,
        name="probe_step",
    )(core.reshape(1), own, other, wave, measured, *tables)


def roll_kernel(meta, illumination, intensities, wave, measured, raw, sem):
    copy = pltpu.make_async_copy(intensities.at[meta[2]], raw, sem)
    copy.start()
    at0 = lax.broadcasted_iota(jnp.int32, (FRAME, FRAME), 0)
    at1 = lax.broadcasted_iota(jnp.int32, (FRAME, FRAME), 1)
    cols = jnp.where(((natural(at0) - meta[1]) & (FRAME - 1)) == at1, 1.0, 0.0).astype(BF)
    rows = jnp.where(((natural(at1) - meta[0]) & (FRAME - 1)) == at0, 1.0, 0.0).astype(BF)
    for part in range(2):
        turned = lax.dot_general(cols, illumination[part], (NT, ((), ())), preferred_element_type=F32)
        wave[part] = jnp.dot(turned.astype(BF), rows, preferred_element_type=F32).astype(BF)
    copy.wait()
    measured[...] = raw[...].T


def roll_step(meta, illumination, intensities):
    return pl.pallas_call(
        roll_kernel,
        out_shape=(
            jax.ShapeDtypeStruct((2, FRAME, FRAME), BF),
            jax.ShapeDtypeStruct((FRAME, FRAME), F32),
        ),
        in_specs=[SM, VM, ANY],
        out_specs=(VM, VM),
        scratch_shapes=[pltpu.VMEM((FRAME, FRAME), F32), pltpu.SemaphoreType.DMA],
        compiler_params=PARAMS,
        name="roll_step",
    )(meta, illumination, intensities)


def sum_kernel(meta, parts, out, acc):
    core, base = meta[128], meta[129]
    acc[...] = jnp.zeros(acc.shape, F32)
    at0 = lax.broadcasted_iota(jnp.int32, (8, 128), 0)
    at1 = lax.broadcasted_iota(jnp.int32, (8, 128), 1)
    column = base + at0
    row = [natural(256 * c + 128 * core + at1) for c in range(2)]

    def step(k, _):
        top, edge = meta[k] >> 9, meta[k] & (FRAME - 1)
        right = column < meta[64 + k]
        for c in range(2):
            below = row[c] < edge
            for plane in range(4):
                g = parts[k, c, plane].astype(F32)
                for tile, piece in ((top, jnp.where(below, 0.0, g)), (top + 1, jnp.where(below, g, 0.0))):
                    acc[0, tile, plane, c] += jnp.where(right, 0.0, piece)
                    acc[1, tile, plane, c] += jnp.where(right, piece, 0.0)
        return 0

    lax.fori_loop(0, 64, step, 0)
    for h in range(2):
        for tile in range(4):
            for plane in range(4):
                for c in range(2):
                    out[4 * h + tile, plane, :, 128 * c : 128 * c + 128] = acc[h, tile, plane, c].astype(BF)


def sum_step(meta, parts):
    return pl.pallas_call(
        sum_kernel,
        out_shape=jax.ShapeDtypeStruct((8, 4, 8, 256), BF),
        in_specs=[SM, VM],
        out_specs=VM,
        scratch_shapes=[pltpu.VMEM((2, 5, 4, 2, 8, 128), F32)],
        compiler_params=PARAMS,
        name="sum_step",
    )(meta, parts)


def body(transmission, illumination, intensities, scan_positions, tile_owner):
    (far_re, far_im), (prop_re, prop_im) = build_tables()
    half, col = lax.axis_index("half"), lax.axis_index("col")
    which, core = lax.axis_index("zl"), lax.axis_index("core")
    my_col = half * 16 + col
    order = jnp.arange(FRAME, dtype=jnp.int32)
    residue = natural(order)

    row0 = tile_owner * TILE_ROWS - BORDER + scan_positions[:, 0]
    col0 = scan_positions[:, 1]
    info = jnp.stack([row0 // 32, row0 % 32, col0 // 32, col0 % 32], axis=1).reshape(8).astype(BF)
    place = (residue[None, :] == order[:, None]).astype(BF)
    block = dot(transmission.reshape(4, 512, 32), place, ((1,), (0,))).astype(BF)
    block = block.reshape(4, 32, 2, 2, 128).transpose(1, 3, 2, 0, 4).reshape(128, 4, 128)
    info = jnp.broadcast_to(jnp.pad(info, (0, 120)), (128, 4, 128))
    got = lax.all_to_all(jnp.concatenate([block, info], axis=1), ALL, 0, 0, tiled=True)

    mine = jnp.stack([row0, col0], axis=1)[which]
    wave, measured = roll_step(jnp.concatenate([mine, which.reshape(1)]), illumination, intensities)
    tables = (
        right_form(prop_re, prop_im),
        right_form(prop_re, -prop_im),
        right_form(far_re, far_im),
        right_form(far_re.T, -far_im.T),
    )
    got, wave, measured = lax.optimization_barrier((got, wave, measured))

    told = got[::4, 4, :8].astype(jnp.int32).reshape(64, 4)
    rows0 = told[:, 0] * 32 + told[:, 1]
    cols0 = told[:, 2] * 32 + told[:, 3]
    cand = got[:, :4].reshape(2, 2, 8, 4, 4, 128).transpose(0, 3, 1, 4, 2, 5)
    column = (jnp.arange(16, dtype=jnp.int32) * 32 + my_col).reshape(2, 8)
    row = natural((2 * core + which) * 128 + jnp.arange(128, dtype=jnp.int32))
    side = (column[None] < cols0[:, None, None]).astype(jnp.int32)
    tile = rows0[:, None] // 512 + (row[None, :] < rows0[:, None] % 512)
    pick = tile[:, None, None, :] + 4 * side[..., None]
    sent = jnp.zeros((64, 2, 4, 8, 128), BF)
    for a in range(2):
        for b in range(4):
            sent = jnp.where((pick == 4 * a + b)[:, :, None], cand[a, b][None], sent)
    own = lax.all_to_all(sent.reshape(128, 4, 8, 128), ALL, 0, 0, tiled=True).reshape(32, 2, 2, 4, 8, 128)
    other = lax.ppermute(own, "core", [(0, 1), (1, 0)])

    grad, loss = probe_step(core, own, other, wave, measured, tables)

    home = lax.all_to_all(grad.reshape(128, 4, 8, 128), ALL, 0, 0, tiled=True)
    base = col * 32 + (half * 2 + which) * 8
    sums = sum_step(jnp.concatenate([rows0, cols0, jnp.stack([core, base])]), home.reshape(64, 2, 4, 8, 128))
    final = lax.all_to_all(sums, SHARERS, 0, 0, tiled=True)
    final = final.reshape(2, 2, 2, 4, 8, 2, 128).transpose(3, 0, 1, 4, 5, 2, 6).reshape(4, 32, 512)
    gradient = lax.dot_general(place, final, (((1,), (2,)), ((), ())), preferred_element_type=F32)
    gradient = gradient.transpose(1, 0, 2).reshape(2, 2, 512, 32)

    loss = loss[0, :1]
    loss_other = lax.ppermute(loss, "zl", [(0, 1), (1, 0)])
    pair = jnp.concatenate([loss, loss_other])
    probe_losses = jnp.where(which == 0, pair, pair[::-1])
    return gradient, probe_losses


def solution(mesh):
    split = Mesh(mesh.devices.reshape(2, 16, 2, 2), ALL)
    tile = ("zl", "core")
    return jax.shard_map(
        body,
        mesh=split,
        in_specs=(
            P(None, None, tile, PROBE),
            P(),
            P(PROBE, None, None),
            P(PROBE, None),
            P(PROBE),
        ),
        out_specs=(P(None, None, tile, PROBE), P(PROBE)),
        check_vma=False,
    )
```

```python
import math

import jax
import jax.numpy as jnp
import numpy as np
from jax import lax
from jax.experimental import pallas as pl
from jax.experimental.pallas import tpu as pltpu
from jax.sharding import Mesh
from jax.sharding import PartitionSpec as P

FRAME = 512
BORDER = 128
TILE_ROWS = 512
FRESNEL = 0.25
PROBE = ("half", "col")
CHIPS = ("half", "col", "zl")
ALL = ("half", "col", "zl", "core")
SHARERS = ("half", "zl", "core")
BF = jnp.bfloat16
F32 = jnp.float32


def natural(order):
    return order % 16 * 32 + order // 16


def build_tables():
    n = FRAME
    index = np.arange(n)
    angle = (np.float32(-2.0 * math.pi) * (np.outer(index, index) % n).astype(np.float32) / np.float32(n)).astype(np.float32)
    norm = np.float32(1.0 / math.sqrt(n))
    wave_re, wave_im = np.cos(angle) * norm, np.sin(angle) * norm
    freq = np.where(index < n // 2, index, index - n).astype(np.float32)
    phase = (np.float32(-math.pi * FRESNEL) * freq * freq / np.float32(n)).astype(np.float32)
    kre, kim = np.cos(phase)[:, None], np.sin(phase)[:, None]
    sre, sim = kre * wave_re - kim * wave_im, kre * wave_im + kim * wave_re
    prop_re = wave_re @ sre + wave_im @ sim
    prop_im = wave_re @ sim - wave_im @ sre
    perm = natural(index)
    bf = jnp.bfloat16
    far = (wave_re[perm].astype(bf), wave_im[perm].astype(bf))
    prop = (prop_re[perm][:, perm].astype(bf), prop_im[perm][:, perm].astype(bf))
    return far, prop


def right_form(re, im):
    re, im = jnp.asarray(re), jnp.asarray(im)
    return jnp.concatenate([jnp.concatenate([re, im], 1), jnp.concatenate([-im, re], 1)], 0)


def dot(left, right, dims):
    return lax.dot_general(left, right, (dims, ((), ())), preferred_element_type=F32)


NN = ((1,), (0,))
NT = ((1,), (1,))


def probe_kernel(
    core_ref, own, other, wave, measured_hbm, bq_hbm, aq_hbm, bw_hbm, aw_hbm, out, loss,
    y, inner, x1, field, turn, measured, bq, aq, bw, aw, sems,
):
    copies = [
        pltpu.make_async_copy(src, dst, sems.at[n])
        for n, (src, dst) in enumerate(
            ((bq_hbm, bq), (aq_hbm, aq), (bw_hbm, bw), (aw_hbm, aw), (measured_hbm, measured))
        )
    ]
    for copy in copies:
        copy.start()
    core = core_ref[0]
    first = core == 0
    here = pl.multiple_of(core * 256, 256)

    def layer(i, z, c, plane):
        mine, rest = own[i, z, c, plane].astype(F32), other[i, z, c, plane].astype(F32)
        return jnp.concatenate([jnp.where(first, mine, rest), jnp.where(first, rest, mine)], axis=0)

    def block_rows(i):
        return pl.ds(pl.multiple_of(i * 16, 16), 16), pl.ds(pl.multiple_of(512 + i * 16, 16), 16)

    def product(plane, get, conj):
        def step(i, _):
            rows, _ = block_rows(i)
            for z in range(2):
                for c in range(2):
                    at = 256 * c + 128 * z
                    ore, oim = layer(i, z, c, plane), layer(i, z, c, plane + 1)
                    vre, vim = get(i, slice(at, at + 128))
                    if conj:
                        re, im = ore * vre + oim * vim, ore * vim - oim * vre
                    else:
                        re, im = ore * vre - oim * vim, ore * vim + oim * vre
                    y[rows, at : at + 128] = re.astype(BF)
                    y[rows, 512 + at : 640 + at] = im.astype(BF)
            return 0

        lax.fori_loop(0, 32, step, 0, unroll=2)

    def from_wave(i, lanes):
        rows, _ = block_rows(i)
        return wave[0, rows, lanes].astype(F32), wave[1, rows, lanes].astype(F32)

    def from_ref(ref):
        def get(i, lanes):
            rows, rows_im = block_rows(i)
            return ref[rows, lanes], ref[rows_im, lanes]

        return get

    def right(table):
        for n in range(4):
            got = jnp.dot(y[...], table[:, n * 256 : n * 256 + 256], preferred_element_type=F32)
            inner[n // 2 * 512 : n // 2 * 512 + 512, n % 2 * 256 : n % 2 * 256 + 256] = got.astype(BF)

    def left(table, dst):
        for n in range(2):
            dst[:, n * 256 : n * 256 + 256] = jnp.dot(
                table[...], inner[:, n * 256 : n * 256 + 256], preferred_element_type=F32
            )

    def hand_out(plane):
        for o in range(4):
            for j in range(16):
                for part in range(2):
                    rows = pl.ds(part * 512 + 128 * o + j, 8, stride=16)
                    for z in range(2):
                        out[o // 2, j, o % 2, z, plane + part] = turn[z, rows, :].astype(BF)

    product(0, from_wave, False)
    copies[0].wait()
    right(bq)
    copies[1].wait()
    left(aq, x1)
    product(2, from_ref(x1), False)
    copies[2].wait()
    right(bw)
    copies[3].wait()
    left(aw, field)
    copies[4].wait()

    def compare(i, total):
        rows, rows_im = block_rows(i)
        re, im = field[rows, :], field[rows_im, :]
        misfit = re * re + im * im - measured[rows, :]
        y[rows, 0:512] = (misfit * re).astype(BF)
        y[rows, 512:1024] = (misfit * im).astype(BF)
        return total + misfit * misfit

    total = lax.fori_loop(0, 32, compare, jnp.zeros((16, 512), F32))
    loss[...] = jnp.full((8, 128), jnp.sum(total) * (1.0 / (FRAME * FRAME)), F32)
    right(aw)
    left(bw, field)
    product(2, from_ref(field), True)

    def gradient1(i, _):
        rows, rows_im = block_rows(i)
        for z in range(2):
            lanes = pl.ds(pl.multiple_of(here + z * 128, 128), 128)
            bre, bim = field[rows, lanes], field[rows_im, lanes]
            xre, xim = x1[rows, lanes], x1[rows_im, lanes]
            turn[z, rows, :] = xre * bre + xim * bim
            turn[z, rows_im, :] = xre * bim - xim * bre
        return 0

    lax.fori_loop(0, 32, gradient1, 0, unroll=2)
    hand_out(2)
    for part in range(2):
        cols = pl.ds(pl.multiple_of(here + part * 512, 256), 256)
        got = jnp.dot(y[...], aq[:, cols], preferred_element_type=F32)
        inner[part * 512 : part * 512 + 512, 0:256] = got.astype(BF)
    field[:, 0:256] = jnp.dot(bq[...], inner[:, 0:256], preferred_element_type=F32)

    def gradient0(i, _):
        rows, rows_im = block_rows(i)
        for z in range(2):
            bre, bim = field[rows, z * 128 : z * 128 + 128], field[rows_im, z * 128 : z * 128 + 128]
            xre, xim = from_wave(i, pl.ds(pl.multiple_of(here + z * 128, 128), 128))
            turn[z, rows, :] = xre * bre + xim * bim
            turn[z, rows_im, :] = xre * bim - xim * bre
        return 0

    lax.fori_loop(0, 32, gradient0, 0, unroll=2)
    hand_out(0)


VM = pl.BlockSpec(memory_space=pltpu.VMEM)
SM = pl.BlockSpec(memory_space=pltpu.SMEM)
ANY = pl.BlockSpec(memory_space=pl.ANY)
PARAMS = pltpu.CompilerParams(vmem_limit_bytes=56 * 2**20)


def placed(value):
    return pltpu.with_memory_space_constraint(value, pltpu.VMEM)


def probe_step(core, own, other, wave, measured, tables):
    return pl.pallas_call(
        probe_kernel,
        out_shape=(
            pltpu.VMEM((2, 16, 2, 2, 4, 8, 128), BF),
            jax.ShapeDtypeStruct((8, 128), F32),
        ),
        in_specs=[SM, VM, VM, VM] + [ANY] * 5,
        out_specs=(VM, VM),
        scratch_shapes=[
            pltpu.VMEM((512, 1024), BF),
            pltpu.VMEM((1024, 512), BF),
            pltpu.VMEM((1024, 512), F32),
            pltpu.VMEM((1024, 512), F32),
            pltpu.VMEM((2, 1024, 128), F32),
            pltpu.VMEM((512, 512), F32),
        ]
        + [pltpu.VMEM((1024, 1024), BF)] * 4
        + [pltpu.SemaphoreType.DMA((5,))],
        compiler_params=PARAMS,
        name="probe_step",
    )(core.reshape(1), placed(own), placed(other), placed(wave), measured, *tables)


def corner(positions, owner, k):
    return owner[k] * TILE_ROWS - BORDER + positions[k, 0], positions[k, 1]


def prepare_kernel(positions, owner, block, out, rows):
    at0 = lax.broadcasted_iota(jnp.int32, (FRAME, FRAME), 0)
    at1 = lax.broadcasted_iota(jnp.int32, (FRAME, FRAME), 1)
    place = jnp.where(natural(at1) == at0, 1.0, 0.0).astype(BF)
    got = jnp.dot(block[...], place, preferred_element_type=F32)
    lane = lax.broadcasted_iota(jnp.int32, (128, 128), 1)
    info = jnp.zeros((128, 128), jnp.int32)
    for k in range(2):
        for n, value in enumerate(corner(positions, owner, k)):
            info = jnp.where(lane == 4 * k + 2 * n, value >> 5, info)
            info = jnp.where(lane == 4 * k + 2 * n + 1, value & 31, info)
    for q in range(4):
        rows[q, 0:128] = got[:, q * 128 : q * 128 + 128]
        rows[q, 128:256] = info.astype(F32)
    for i in range(32):
        for q in range(4):
            out[i, q % 2, q // 2] = rows[q, pl.ds(i, 8, stride=32), :].astype(BF)


def prepare_step(positions, owner, block):
    return pl.pallas_call(
        prepare_kernel,
        out_shape=pltpu.VMEM((32, 2, 2, 8, 128), BF),
        in_specs=[SM, SM, VM],
        out_specs=VM,
        scratch_shapes=[pltpu.VMEM((4, 256, 128), F32)],
        compiler_params=PARAMS,
        name="prepare_step",
    )(positions, owner, block)


def roll_kernel(positions, owner, which, illumination, intensities, wave, measured, raw, sem):
    copy = pltpu.make_async_copy(intensities.at[which[0]], raw, sem)
    copy.start()
    row0, col0 = corner(positions, owner, which[0])
    at0 = lax.broadcasted_iota(jnp.int32, (FRAME, FRAME), 0)
    at1 = lax.broadcasted_iota(jnp.int32, (FRAME, FRAME), 1)
    cols = jnp.where(((natural(at0) - col0) & (FRAME - 1)) == at1, 1.0, 0.0).astype(BF)
    rows = jnp.where(((natural(at1) - row0) & (FRAME - 1)) == at0, 1.0, 0.0).astype(BF)
    for part in range(2):
        turned = lax.dot_general(cols, illumination[part], (NT, ((), ())), preferred_element_type=F32)
        wave[part] = jnp.dot(turned.astype(BF), rows, preferred_element_type=F32).astype(BF)
    copy.wait()
    measured[...] = raw[...].T


def roll_step(positions, owner, which, illumination, intensities):
    return pl.pallas_call(
        roll_kernel,
        out_shape=(
            pltpu.VMEM((2, FRAME, FRAME), BF),
            jax.ShapeDtypeStruct((FRAME, FRAME), F32),
        ),
        in_specs=[SM, SM, SM, VM, ANY],
        out_specs=(VM, VM),
        scratch_shapes=[pltpu.VMEM((FRAME, FRAME), F32), pltpu.SemaphoreType.DMA],
        compiler_params=PARAMS,
        name="roll_step",
    )(positions, owner, which.reshape(1), illumination, intensities)


def sum_kernel(meta, parts, out, acc):
    core, base = meta[128], meta[129]
    acc[...] = jnp.zeros(acc.shape, F32)
    at0 = lax.broadcasted_iota(jnp.int32, (8, 128), 0)
    at1 = lax.broadcasted_iota(jnp.int32, (8, 128), 1)
    column = base + at0
    row = [natural(256 * c + 128 * core + at1) for c in range(2)]

    def step(k, _):
        top, edge = meta[k] >> 9, meta[k] & (FRAME - 1)
        right = column < meta[64 + k]
        for c in range(2):
            below = row[c] < edge
            for plane in range(4):
                g = parts[k, c, plane].astype(F32)
                for tile, piece in ((top, jnp.where(below, 0.0, g)), (top + 1, jnp.where(below, g, 0.0))):
                    acc[0, tile, plane, c] += jnp.where(right, 0.0, piece)
                    acc[1, tile, plane, c] += jnp.where(right, piece, 0.0)
        return 0

    lax.fori_loop(0, 64, step, 0)
    for h in range(2):
        for tile in range(4):
            for plane in range(4):
                for c in range(2):
                    out[4 * h + tile, plane, :, 128 * c : 128 * c + 128] = acc[h, tile, plane, c].astype(BF)


def sum_step(meta, parts):
    return pl.pallas_call(
        sum_kernel,
        out_shape=pltpu.VMEM((8, 4, 8, 256), BF),
        in_specs=[SM, VM],
        out_specs=VM,
        scratch_shapes=[pltpu.VMEM((2, 5, 4, 2, 8, 128), F32)],
        compiler_params=PARAMS,
        name="sum_step",
    )(meta, placed(parts))


def body(transmission, illumination, intensities, scan_positions, tile_owner):
    (far_re, far_im), (prop_re, prop_im) = build_tables()
    half, col = lax.axis_index("half"), lax.axis_index("col")
    which, core = lax.axis_index("zl"), lax.axis_index("core")
    my_col = half * 16 + col
    order = jnp.arange(FRAME, dtype=jnp.int32)
    residue = natural(order)

    place = (residue[None, :] == order[:, None]).astype(BF)
    block = placed(transmission.transpose(0, 1, 3, 2).reshape(128, 512))
    sent = prepare_step(scan_positions, tile_owner, block)
    got = lax.all_to_all(sent.reshape(128, 8, 128), ALL, 0, 0, tiled=True)

    wave, measured = roll_step(scan_positions, tile_owner, which, illumination, intensities)
    tables = (
        right_form(prop_re, prop_im),
        right_form(prop_re, -prop_im),
        right_form(far_re, far_im),
        right_form(far_re.T, -far_im.T),
    )
    got, wave, measured = lax.optimization_barrier((got, wave, measured))

    told = got[::4, 4, :8].astype(jnp.int32).reshape(64, 4)
    rows0 = told[:, 0] * 32 + told[:, 1]
    cols0 = told[:, 2] * 32 + told[:, 3]
    cand = got[:, :4].reshape(2, 2, 8, 4, 4, 128).transpose(0, 3, 1, 4, 2, 5)
    column = (jnp.arange(16, dtype=jnp.int32) * 32 + my_col).reshape(2, 8)
    row = natural((2 * core + which) * 128 + jnp.arange(128, dtype=jnp.int32))
    side = (column[None] < cols0[:, None, None]).astype(jnp.int32)
    tile = rows0[:, None] // 512 + (row[None, :] < rows0[:, None] % 512)
    pick = tile[:, None, None, :] + 4 * side[..., None]
    sent = jnp.zeros((64, 2, 4, 8, 128), BF)
    for a in range(2):
        for b in range(4):
            sent = jnp.where((pick == 4 * a + b)[:, :, None], cand[a, b][None], sent)
    own = lax.all_to_all(sent.reshape(128, 4, 8, 128), ALL, 0, 0, tiled=True).reshape(32, 2, 2, 4, 8, 128)
    other = lax.ppermute(own, "core", [(0, 1), (1, 0)])

    grad, loss = probe_step(core, own, other, wave, measured, tables)

    home = lax.all_to_all(grad.reshape(128, 4, 8, 128), ALL, 0, 0, tiled=True)
    base = col * 32 + (half * 2 + which) * 8
    sums = sum_step(jnp.concatenate([rows0, cols0, jnp.stack([core, base])]), home.reshape(64, 2, 4, 8, 128))
    final = lax.all_to_all(sums, SHARERS, 0, 0, tiled=True)
    final = final.reshape(2, 2, 2, 4, 8, 2, 128).transpose(3, 0, 1, 4, 5, 2, 6).reshape(4, 32, 512)
    gradient = lax.dot_general(place, final, (((1,), (2,)), ((), ())), preferred_element_type=F32)
    gradient = gradient.transpose(1, 0, 2).reshape(2, 2, 512, 32)

    loss = loss[0, :1]
    loss_other = lax.ppermute(loss, "zl", [(0, 1), (1, 0)])
    pair = jnp.concatenate([loss, loss_other])
    probe_losses = jnp.where(which == 0, pair, pair[::-1])
    return gradient, probe_losses


def solution(mesh):
    split = Mesh(mesh.devices.reshape(2, 16, 2, 2), ALL)
    tile = ("zl", "core")
    return jax.shard_map(
        body,
        mesh=split,
        in_specs=(
            P(None, None, tile, PROBE),
            P(),
            P(PROBE, None, None),
            P(PROBE, None),
            P(PROBE),
        ),
        out_specs=(P(None, None, tile, PROBE), P(PROBE)),
        check_vma=False,
    )
```

```python
import math

import jax
import jax.numpy as jnp
import numpy as np
from jax import lax
from jax.experimental import pallas as pl
from jax.experimental.pallas import tpu as pltpu
from jax.sharding import Mesh
from jax.sharding import PartitionSpec as P

FRAME = 512
BORDER = 128
TILE_ROWS = 512
FRESNEL = 0.25
PROBE = ("half", "col")
CHIPS = ("half", "col", "zl")
ALL = ("half", "col", "zl", "core")
SHARERS = ("half", "zl", "core")
BF = jnp.bfloat16
F32 = jnp.float32


def natural(order):
    return order % 16 * 32 + order // 16


def build_tables():
    n = FRAME
    index = np.arange(n)
    angle = (np.float32(-2.0 * math.pi) * (np.outer(index, index) % n).astype(np.float32) / np.float32(n)).astype(np.float32)
    norm = np.float32(1.0 / math.sqrt(n))
    wave_re, wave_im = np.cos(angle) * norm, np.sin(angle) * norm
    freq = np.where(index < n // 2, index, index - n).astype(np.float32)
    phase = (np.float32(-math.pi * FRESNEL) * freq * freq / np.float32(n)).astype(np.float32)
    kre, kim = np.cos(phase)[:, None], np.sin(phase)[:, None]
    sre, sim = kre * wave_re - kim * wave_im, kre * wave_im + kim * wave_re
    prop_re = wave_re @ sre + wave_im @ sim
    prop_im = wave_re @ sim - wave_im @ sre
    perm = natural(index)
    bf = jnp.bfloat16
    far = (wave_re[perm].astype(bf), wave_im[perm].astype(bf))
    prop = (prop_re[perm][:, perm].astype(bf), prop_im[perm][:, perm].astype(bf))
    return far, prop


def right_form(re, im):
    re, im = jnp.asarray(re), jnp.asarray(im)
    return jnp.concatenate([jnp.concatenate([re, im], 1), jnp.concatenate([-im, re], 1)], 0)


def dot(left, right, dims):
    return lax.dot_general(left, right, (dims, ((), ())), preferred_element_type=F32)


NN = ((1,), (0,))
NT = ((1,), (1,))


def probe_kernel(
    core_ref, own, other, wave, bq, measured_hbm, aq_hbm, bw_hbm, aw_hbm, out, loss,
    y, inner, x1, field, turn, measured, aq, bw, aw, sems,
):
    copies = [
        pltpu.make_async_copy(src, dst, sems.at[n])
        for n, (src, dst) in enumerate(
            ((aq_hbm, aq), (bw_hbm, bw), (aw_hbm, aw), (measured_hbm, measured))
        )
    ]
    copies[0].start()
    core = core_ref[0]
    first = core == 0
    here = pl.multiple_of(core * 256, 256)

    def layer(i, z, c, plane):
        mine, rest = own[i, z, c, plane].astype(F32), other[i, z, c, plane].astype(F32)
        return jnp.concatenate([jnp.where(first, mine, rest), jnp.where(first, rest, mine)], axis=0)

    def block_rows(i):
        return pl.ds(pl.multiple_of(i * 16, 16), 16), pl.ds(pl.multiple_of(512 + i * 16, 16), 16)

    def product(plane, get, conj):
        def step(i, _):
            rows, _ = block_rows(i)
            for z in range(2):
                for c in range(2):
                    at = 256 * c + 128 * z
                    ore, oim = layer(i, z, c, plane), layer(i, z, c, plane + 1)
                    vre, vim = get(i, slice(at, at + 128))
                    if conj:
                        re, im = ore * vre + oim * vim, ore * vim - oim * vre
                    else:
                        re, im = ore * vre - oim * vim, ore * vim + oim * vre
                    y[rows, at : at + 128] = re.astype(BF)
                    y[rows, 512 + at : 640 + at] = im.astype(BF)
            return 0

        lax.fori_loop(0, 32, step, 0, unroll=2)

    def from_wave(i, lanes):
        rows, _ = block_rows(i)
        return wave[0, rows, lanes].astype(F32), wave[1, rows, lanes].astype(F32)

    def from_ref(ref):
        def get(i, lanes):
            rows, rows_im = block_rows(i)
            return ref[rows, lanes], ref[rows_im, lanes]

        return get

    def right(table):
        for n in range(4):
            got = jnp.dot(y[...], table[:, n * 256 : n * 256 + 256], preferred_element_type=F32)
            inner[n // 2 * 512 : n // 2 * 512 + 512, n % 2 * 256 : n % 2 * 256 + 256] = got.astype(BF)

    def left(table, dst):
        for n in range(4):
            rows = slice(n * 256, n * 256 + 256)
            dst[rows, :] = jnp.dot(table[rows, :], inner[...], preferred_element_type=F32)

    def hand_out(plane):
        for o in range(4):
            for j in range(16):
                for part in range(2):
                    rows = pl.ds(part * 512 + 128 * o + j, 8, stride=16)
                    for z in range(2):
                        out[o // 2, j, o % 2, z, plane + part] = turn[z, rows, :].astype(BF)

    product(0, from_wave, False)
    right(bq)
    copies[0].wait()
    for copy in copies[1:]:
        copy.start()
    left(aq, x1)
    product(2, from_ref(x1), False)
    copies[1].wait()
    right(bw)
    copies[2].wait()
    left(aw, field)
    copies[3].wait()

    def compare(i, total):
        rows, rows_im = block_rows(i)
        re, im = field[rows, :], field[rows_im, :]
        misfit = re * re + im * im - measured[rows, :]
        y[rows, 0:512] = (misfit * re).astype(BF)
        y[rows, 512:1024] = (misfit * im).astype(BF)
        return total + misfit * misfit

    total = lax.fori_loop(0, 32, compare, jnp.zeros((16, 512), F32))
    loss[...] = jnp.full((8, 128), jnp.sum(total) * (1.0 / (FRAME * FRAME)), F32)
    right(aw)
    left(bw, field)
    product(2, from_ref(field), True)

    def gradient1(i, _):
        rows, rows_im = block_rows(i)
        for z in range(2):
            lanes = pl.ds(pl.multiple_of(here + z * 128, 128), 128)
            bre, bim = field[rows, lanes], field[rows_im, lanes]
            xre, xim = x1[rows, lanes], x1[rows_im, lanes]
            turn[z, rows, :] = xre * bre + xim * bim
            turn[z, rows_im, :] = xre * bim - xim * bre
        return 0

    lax.fori_loop(0, 32, gradient1, 0, unroll=2)
    hand_out(2)
    for part in range(2):
        cols = pl.ds(pl.multiple_of(here + part * 512, 256), 256)
        got = jnp.dot(y[...], aq[:, cols], preferred_element_type=F32)
        inner[part * 512 : part * 512 + 512, 0:256] = got.astype(BF)
    for n in range(4):
        rows = slice(n * 256, n * 256 + 256)
        field[rows, 0:256] = jnp.dot(bq[rows, :], inner[:, 0:256], preferred_element_type=F32)

    def gradient0(i, _):
        rows, rows_im = block_rows(i)
        for z in range(2):
            bre, bim = field[rows, z * 128 : z * 128 + 128], field[rows_im, z * 128 : z * 128 + 128]
            xre, xim = from_wave(i, pl.ds(pl.multiple_of(here + z * 128, 128), 128))
            turn[z, rows, :] = xre * bre + xim * bim
            turn[z, rows_im, :] = xre * bim - xim * bre
        return 0

    lax.fori_loop(0, 32, gradient0, 0, unroll=2)
    hand_out(0)


VM = pl.BlockSpec(memory_space=pltpu.VMEM)
SM = pl.BlockSpec(memory_space=pltpu.SMEM)
ANY = pl.BlockSpec(memory_space=pl.ANY)
PARAMS = pltpu.CompilerParams(vmem_limit_bytes=56 * 2**20)


def placed(value):
    return pltpu.with_memory_space_constraint(value, pltpu.VMEM)


def probe_step(core, own, other, wave, measured, tables):
    return pl.pallas_call(
        probe_kernel,
        out_shape=(
            pltpu.VMEM((2, 16, 2, 2, 4, 8, 128), BF),
            jax.ShapeDtypeStruct((8, 128), F32),
        ),
        in_specs=[SM] + [VM] * 4 + [ANY] * 4,
        out_specs=(VM, VM),
        scratch_shapes=[
            pltpu.VMEM((512, 1024), BF),
            pltpu.VMEM((1024, 512), BF),
            pltpu.VMEM((1024, 512), F32),
            pltpu.VMEM((1024, 512), F32),
            pltpu.VMEM((2, 1024, 128), F32),
            pltpu.VMEM((512, 512), F32),
        ]
        + [pltpu.VMEM((1024, 1024), BF)] * 3
        + [pltpu.SemaphoreType.DMA((4,))],
        compiler_params=PARAMS,
        name="probe_step",
    )(core.reshape(1), placed(own), placed(other), placed(wave), placed(tables[0]), measured, *tables[1:])


def corner(positions, owner, k):
    return owner[k] * TILE_ROWS - BORDER + positions[k, 0], positions[k, 1]


def prepare_kernel(positions, owner, block, out, rows):
    at0 = lax.broadcasted_iota(jnp.int32, (FRAME, FRAME), 0)
    at1 = lax.broadcasted_iota(jnp.int32, (FRAME, FRAME), 1)
    place = jnp.where(natural(at1) == at0, 1.0, 0.0).astype(BF)
    got = jnp.dot(block[...], place, preferred_element_type=F32)
    lane = lax.broadcasted_iota(jnp.int32, (128, 128), 1)
    info = jnp.zeros((128, 128), jnp.int32)
    for k in range(2):
        for n, value in enumerate(corner(positions, owner, k)):
            info = jnp.where(lane == 4 * k + 2 * n, value >> 5, info)
            info = jnp.where(lane == 4 * k + 2 * n + 1, value & 31, info)
    for q in range(4):
        rows[q, 0:128] = got[:, q * 128 : q * 128 + 128]
        rows[q, 128:256] = info.astype(F32)
    for i in range(32):
        for q in range(4):
            out[i, q % 2, q // 2] = rows[q, pl.ds(i, 8, stride=32), :].astype(BF)


def prepare_step(positions, owner, block):
    return pl.pallas_call(
        prepare_kernel,
        out_shape=pltpu.VMEM((32, 2, 2, 8, 128), BF),
        in_specs=[SM, SM, VM],
        out_specs=VM,
        scratch_shapes=[pltpu.VMEM((4, 256, 128), F32)],
        compiler_params=PARAMS,
        name="prepare_step",
    )(positions, owner, block)


def roll_kernel(positions, owner, which, illumination, intensities, wave, measured, raw, sem):
    copy = pltpu.make_async_copy(intensities.at[which[0]], raw, sem)
    copy.start()
    row0, col0 = corner(positions, owner, which[0])
    at0 = lax.broadcasted_iota(jnp.int32, (FRAME, FRAME), 0)
    at1 = lax.broadcasted_iota(jnp.int32, (FRAME, FRAME), 1)
    cols = jnp.where(((natural(at0) - col0) & (FRAME - 1)) == at1, 1.0, 0.0).astype(BF)
    rows = jnp.where(((natural(at1) - row0) & (FRAME - 1)) == at0, 1.0, 0.0).astype(BF)
    for part in range(2):
        turned = lax.dot_general(cols, illumination[part], (NT, ((), ())), preferred_element_type=F32)
        wave[part] = jnp.dot(turned.astype(BF), rows, preferred_element_type=F32).astype(BF)
    copy.wait()
    measured[...] = raw[...].T


def roll_step(positions, owner, which, illumination, intensities):
    return pl.pallas_call(
        roll_kernel,
        out_shape=(
            pltpu.VMEM((2, FRAME, FRAME), BF),
            jax.ShapeDtypeStruct((FRAME, FRAME), F32),
        ),
        in_specs=[SM, SM, SM, VM, ANY],
        out_specs=(VM, VM),
        scratch_shapes=[pltpu.VMEM((FRAME, FRAME), F32), pltpu.SemaphoreType.DMA],
        compiler_params=PARAMS,
        name="roll_step",
    )(positions, owner, which.reshape(1), illumination, intensities)


def sum_kernel(meta, parts, out, acc):
    core, base = meta[128], meta[129]
    acc[...] = jnp.zeros(acc.shape, F32)
    at0 = lax.broadcasted_iota(jnp.int32, (8, 128), 0)
    at1 = lax.broadcasted_iota(jnp.int32, (8, 128), 1)
    column = base + at0
    row = [natural(256 * c + 128 * core + at1) for c in range(2)]

    def step(k, _):
        top, edge = meta[k] >> 9, meta[k] & (FRAME - 1)
        right = column < meta[64 + k]
        for c in range(2):
            below = row[c] < edge
            for plane in range(4):
                g = parts[k, c, plane].astype(F32)
                for tile, piece in ((top, jnp.where(below, 0.0, g)), (top + 1, jnp.where(below, g, 0.0))):
                    acc[0, tile, plane, c] += jnp.where(right, 0.0, piece)
                    acc[1, tile, plane, c] += jnp.where(right, piece, 0.0)
        return 0

    lax.fori_loop(0, 64, step, 0, unroll=4)
    for h in range(2):
        for tile in range(4):
            for plane in range(4):
                for c in range(2):
                    out[4 * h + tile, plane, :, 128 * c : 128 * c + 128] = acc[h, tile, plane, c].astype(BF)


def sum_step(meta, parts):
    return pl.pallas_call(
        sum_kernel,
        out_shape=pltpu.VMEM((8, 4, 8, 256), BF),
        in_specs=[SM, VM],
        out_specs=VM,
        scratch_shapes=[pltpu.VMEM((2, 5, 4, 2, 8, 128), F32)],
        compiler_params=PARAMS,
        name="sum_step",
    )(meta, placed(parts))


def body(transmission, illumination, intensities, scan_positions, tile_owner):
    (far_re, far_im), (prop_re, prop_im) = build_tables()
    half, col = lax.axis_index("half"), lax.axis_index("col")
    which, core = lax.axis_index("zl"), lax.axis_index("core")
    my_col = half * 16 + col
    order = jnp.arange(FRAME, dtype=jnp.int32)
    residue = natural(order)

    place = (residue[None, :] == order[:, None]).astype(BF)
    block = placed(transmission.transpose(0, 1, 3, 2).reshape(128, 512))
    sent = prepare_step(scan_positions, tile_owner, block)
    got = lax.all_to_all(sent.reshape(128, 8, 128), ALL, 0, 0, tiled=True)

    wave, measured = roll_step(scan_positions, tile_owner, which, illumination, intensities)
    tables = (
        right_form(prop_re, prop_im),
        right_form(prop_re, -prop_im),
        right_form(far_re, far_im),
        right_form(far_re.T, -far_im.T),
    )
    got, wave, measured = lax.optimization_barrier((got, wave, measured))

    told = got[::4, 4, :8].astype(jnp.int32).reshape(64, 4)
    rows0 = told[:, 0] * 32 + told[:, 1]
    cols0 = told[:, 2] * 32 + told[:, 3]
    cand = got[:, :4].reshape(2, 2, 8, 4, 4, 128).transpose(0, 3, 1, 4, 2, 5)
    column = (jnp.arange(16, dtype=jnp.int32) * 32 + my_col).reshape(2, 8)
    row = natural((2 * core + which) * 128 + jnp.arange(128, dtype=jnp.int32))
    side = (column[None] < cols0[:, None, None]).astype(jnp.int32)
    tile = rows0[:, None] // 512 + (row[None, :] < rows0[:, None] % 512)
    pick = tile[:, None, None, :] + 4 * side[..., None]
    sent = jnp.zeros((64, 2, 4, 8, 128), BF)
    for a in range(2):
        for b in range(4):
            sent = jnp.where((pick == 4 * a + b)[:, :, None], cand[a, b][None], sent)
    own = lax.all_to_all(sent.reshape(128, 4, 8, 128), ALL, 0, 0, tiled=True).reshape(32, 2, 2, 4, 8, 128)
    other = lax.ppermute(own, "core", [(0, 1), (1, 0)])

    grad, loss = probe_step(core, own, other, wave, measured, tables)

    home = lax.all_to_all(grad.reshape(128, 4, 8, 128), ALL, 0, 0, tiled=True)
    base = col * 32 + (half * 2 + which) * 8
    sums = sum_step(jnp.concatenate([rows0, cols0, jnp.stack([core, base])]), home.reshape(64, 2, 4, 8, 128))
    final = lax.all_to_all(sums, SHARERS, 0, 0, tiled=True)
    final = final.reshape(2, 2, 2, 4, 8, 2, 128).transpose(3, 0, 1, 4, 5, 2, 6).reshape(4, 32, 512)
    gradient = lax.dot_general(place, final, (((1,), (2,)), ((), ())), preferred_element_type=F32)
    gradient = gradient.transpose(1, 0, 2).reshape(2, 2, 512, 32)

    loss = loss[0, :1]
    loss_other = lax.ppermute(loss, "zl", [(0, 1), (1, 0)])
    pair = jnp.concatenate([loss, loss_other])
    probe_losses = jnp.where(which == 0, pair, pair[::-1])
    return gradient, probe_losses


def solution(mesh):
    split = Mesh(mesh.devices.reshape(2, 16, 2, 2), ALL)
    tile = ("zl", "core")
    return jax.shard_map(
        body,
        mesh=split,
        in_specs=(
            P(None, None, tile, PROBE),
            P(),
            P(PROBE, None, None),
            P(PROBE, None),
            P(PROBE),
        ),
        out_specs=(P(None, None, tile, PROBE), P(PROBE)),
        check_vma=False,
    )
```

```python
import math

import jax
import jax.numpy as jnp
import numpy as np
from jax import lax
from jax.experimental import pallas as pl
from jax.experimental.pallas import tpu as pltpu
from jax.sharding import Mesh
from jax.sharding import PartitionSpec as P

FRAME = 512
BORDER = 128
TILE_ROWS = 512
FRESNEL = 0.25
PROBE = ("half", "col")
CHIPS = ("half", "col", "zl")
ALL = ("half", "col", "zl", "core")
SHARERS = ("half", "zl", "core")
BF = jnp.bfloat16
F32 = jnp.float32


def natural(order):
    return order % 16 * 32 + order // 16


def build_tables():
    n = FRAME
    index = np.arange(n)
    angle = (np.float32(-2.0 * math.pi) * (np.outer(index, index) % n).astype(np.float32) / np.float32(n)).astype(np.float32)
    norm = np.float32(1.0 / math.sqrt(n))
    wave_re, wave_im = np.cos(angle) * norm, np.sin(angle) * norm
    freq = np.where(index < n // 2, index, index - n).astype(np.float32)
    phase = (np.float32(-math.pi * FRESNEL) * freq * freq / np.float32(n)).astype(np.float32)
    kre, kim = np.cos(phase)[:, None], np.sin(phase)[:, None]
    sre, sim = kre * wave_re - kim * wave_im, kre * wave_im + kim * wave_re
    prop_re = wave_re @ sre + wave_im @ sim
    prop_im = wave_re @ sim - wave_im @ sre
    perm = natural(index)
    bf = jnp.bfloat16
    far = (wave_re[perm].astype(bf), wave_im[perm].astype(bf))
    prop = (prop_re[perm][:, perm].astype(bf), prop_im[perm][:, perm].astype(bf))
    return far, prop


def right_form(re, im):
    re, im = jnp.asarray(re), jnp.asarray(im)
    return jnp.concatenate([jnp.concatenate([re, im], 1), jnp.concatenate([-im, re], 1)], 0)


def dot(left, right, dims):
    return lax.dot_general(left, right, (dims, ((), ())), preferred_element_type=F32)


NN = ((1,), (0,))
NT = ((1,), (1,))


def probe_kernel(
    core_ref, own, other, wave, bq, measured_hbm, aq_hbm, bw_hbm, aw_hbm, out, loss,
    y, inner, x1, field, turn, measured, aq, bw, aw, sems,
):
    copies = [
        pltpu.make_async_copy(src, dst, sems.at[n])
        for n, (src, dst) in enumerate(
            ((aq_hbm, aq), (bw_hbm, bw), (aw_hbm, aw), (measured_hbm, measured))
        )
    ]
    copies[0].start()
    core = core_ref[0]
    first = core == 0
    here = pl.multiple_of(core * 256, 256)

    def layer(i, z, c, plane):
        mine, rest = own[i, z, c, plane].astype(F32), other[i, z, c, plane].astype(F32)
        return jnp.concatenate([jnp.where(first, mine, rest), jnp.where(first, rest, mine)], axis=0)

    def block_rows(i):
        return pl.ds(pl.multiple_of(i * 16, 16), 16), pl.ds(pl.multiple_of(512 + i * 16, 16), 16)

    def product(plane, get, conj):
        def step(i):
            rows, _ = block_rows(i)
            for z in range(2):
                for c in range(2):
                    at = 256 * c + 128 * z
                    ore, oim = layer(i, z, c, plane), layer(i, z, c, plane + 1)
                    vre, vim = get(i, slice(at, at + 128))
                    if conj:
                        re, im = ore * vre + oim * vim, ore * vim - oim * vre
                    else:
                        re, im = ore * vre - oim * vim, ore * vim + oim * vre
                    y[rows, at : at + 128] = re.astype(BF)
                    y[rows, 512 + at : 640 + at] = im.astype(BF)
            return 0

        for i in range(32):
            step(i)

    def from_wave(i, lanes):
        rows, _ = block_rows(i)
        return wave[0, rows, lanes].astype(F32), wave[1, rows, lanes].astype(F32)

    def from_ref(ref):
        def get(i, lanes):
            rows, rows_im = block_rows(i)
            return ref[rows, lanes], ref[rows_im, lanes]

        return get

    def right(table):
        for n in range(4):
            got = jnp.dot(y[...], table[:, n * 256 : n * 256 + 256], preferred_element_type=F32)
            inner[n // 2 * 512 : n // 2 * 512 + 512, n % 2 * 256 : n % 2 * 256 + 256] = got.astype(BF)

    def left(table, dst):
        for n in range(4):
            rows = slice(n * 256, n * 256 + 256)
            dst[rows, :] = jnp.dot(table[rows, :], inner[...], preferred_element_type=F32)

    def hand_out(plane):
        for o in range(4):
            for j in range(16):
                for part in range(2):
                    rows = pl.ds(part * 512 + 128 * o + j, 8, stride=16)
                    for z in range(2):
                        out[o // 2, j, o % 2, z, plane + part] = turn[z, rows, :].astype(BF)

    product(0, from_wave, False)
    right(bq)
    copies[0].wait()
    for copy in copies[1:]:
        copy.start()
    left(aq, x1)
    product(2, from_ref(x1), False)
    copies[1].wait()
    right(bw)
    copies[2].wait()
    left(aw, field)
    copies[3].wait()

    def compare(i, total):
        rows, rows_im = block_rows(i)
        re, im = field[rows, :], field[rows_im, :]
        misfit = re * re + im * im - measured[rows, :]
        y[rows, 0:512] = (misfit * re).astype(BF)
        y[rows, 512:1024] = (misfit * im).astype(BF)
        return total + misfit * misfit

    total = lax.fori_loop(0, 32, compare, jnp.zeros((16, 512), F32))
    loss[...] = jnp.full((8, 128), jnp.sum(total) * (1.0 / (FRAME * FRAME)), F32)
    right(aw)
    left(bw, field)
    product(2, from_ref(field), True)

    def gradient1(i, _):
        rows, rows_im = block_rows(i)
        for z in range(2):
            lanes = pl.ds(pl.multiple_of(here + z * 128, 128), 128)
            bre, bim = field[rows, lanes], field[rows_im, lanes]
            xre, xim = x1[rows, lanes], x1[rows_im, lanes]
            turn[z, rows, :] = xre * bre + xim * bim
            turn[z, rows_im, :] = xre * bim - xim * bre
        return 0

    lax.fori_loop(0, 32, gradient1, 0, unroll=2)
    hand_out(2)
    for part in range(2):
        cols = pl.ds(pl.multiple_of(here + part * 512, 256), 256)
        got = jnp.dot(y[...], aq[:, cols], preferred_element_type=F32)
        inner[part * 512 : part * 512 + 512, 0:256] = got.astype(BF)
    for n in range(4):
        rows = slice(n * 256, n * 256 + 256)
        field[rows, 0:256] = jnp.dot(bq[rows, :], inner[:, 0:256], preferred_element_type=F32)

    def gradient0(i, _):
        rows, rows_im = block_rows(i)
        for z in range(2):
            bre, bim = field[rows, z * 128 : z * 128 + 128], field[rows_im, z * 128 : z * 128 + 128]
            xre, xim = from_wave(i, pl.ds(pl.multiple_of(here + z * 128, 128), 128))
            turn[z, rows, :] = xre * bre + xim * bim
            turn[z, rows_im, :] = xre * bim - xim * bre
        return 0

    lax.fori_loop(0, 32, gradient0, 0, unroll=2)
    hand_out(0)


VM = pl.BlockSpec(memory_space=pltpu.VMEM)
SM = pl.BlockSpec(memory_space=pltpu.SMEM)
ANY = pl.BlockSpec(memory_space=pl.ANY)
PARAMS = pltpu.CompilerParams(vmem_limit_bytes=56 * 2**20)


def placed(value):
    return pltpu.with_memory_space_constraint(value, pltpu.VMEM)


def probe_step(core, own, other, wave, measured, tables):
    return pl.pallas_call(
        probe_kernel,
        out_shape=(
            pltpu.VMEM((2, 16, 2, 2, 4, 8, 128), BF),
            jax.ShapeDtypeStruct((8, 128), F32),
        ),
        in_specs=[SM] + [VM] * 4 + [ANY] * 4,
        out_specs=(VM, VM),
        scratch_shapes=[
            pltpu.VMEM((512, 1024), BF),
            pltpu.VMEM((1024, 512), BF),
            pltpu.VMEM((1024, 512), F32),
            pltpu.VMEM((1024, 512), F32),
            pltpu.VMEM((2, 1024, 128), F32),
            pltpu.VMEM((512, 512), F32),
        ]
        + [pltpu.VMEM((1024, 1024), BF)] * 3
        + [pltpu.SemaphoreType.DMA((4,))],
        compiler_params=PARAMS,
        name="probe_step",
    )(core.reshape(1), placed(own), placed(other), placed(wave), placed(tables[0]), measured, *tables[1:])


def corner(positions, owner, k):
    return owner[k] * TILE_ROWS - BORDER + positions[k, 0], positions[k, 1]


def prepare_kernel(positions, owner, block, out, rows):
    at0 = lax.broadcasted_iota(jnp.int32, (FRAME, FRAME), 0)
    at1 = lax.broadcasted_iota(jnp.int32, (FRAME, FRAME), 1)
    place = jnp.where(natural(at1) == at0, 1.0, 0.0).astype(BF)
    got = jnp.dot(block[...], place, preferred_element_type=F32)
    lane = lax.broadcasted_iota(jnp.int32, (128, 128), 1)
    info = jnp.zeros((128, 128), jnp.int32)
    for k in range(2):
        for n, value in enumerate(corner(positions, owner, k)):
            info = jnp.where(lane == 4 * k + 2 * n, value >> 5, info)
            info = jnp.where(lane == 4 * k + 2 * n + 1, value & 31, info)
    for q in range(4):
        rows[q, 0:128] = got[:, q * 128 : q * 128 + 128]
        rows[q, 128:256] = info.astype(F32)
    for i in range(32):
        for q in range(4):
            out[i, q % 2, q // 2] = rows[q, pl.ds(i, 8, stride=32), :].astype(BF)


def prepare_step(positions, owner, block):
    return pl.pallas_call(
        prepare_kernel,
        out_shape=pltpu.VMEM((32, 2, 2, 8, 128), BF),
        in_specs=[SM, SM, VM],
        out_specs=VM,
        scratch_shapes=[pltpu.VMEM((4, 256, 128), F32)],
        compiler_params=PARAMS,
        name="prepare_step",
    )(positions, owner, block)


def roll_kernel(positions, owner, which, illumination, intensities, wave, measured, raw, sem):
    copy = pltpu.make_async_copy(intensities.at[which[0]], raw, sem)
    copy.start()
    row0, col0 = corner(positions, owner, which[0])
    at0 = lax.broadcasted_iota(jnp.int32, (FRAME, FRAME), 0)
    at1 = lax.broadcasted_iota(jnp.int32, (FRAME, FRAME), 1)
    cols = jnp.where(((natural(at0) - col0) & (FRAME - 1)) == at1, 1.0, 0.0).astype(BF)
    rows = jnp.where(((natural(at1) - row0) & (FRAME - 1)) == at0, 1.0, 0.0).astype(BF)
    for part in range(2):
        turned = lax.dot_general(cols, illumination[part], (NT, ((), ())), preferred_element_type=F32)
        wave[part] = jnp.dot(turned.astype(BF), rows, preferred_element_type=F32).astype(BF)
    copy.wait()
    measured[...] = raw[...].T


def roll_step(positions, owner, which, illumination, intensities):
    return pl.pallas_call(
        roll_kernel,
        out_shape=(
            pltpu.VMEM((2, FRAME, FRAME), BF),
            jax.ShapeDtypeStruct((FRAME, FRAME), F32),
        ),
        in_specs=[SM, SM, SM, VM, ANY],
        out_specs=(VM, VM),
        scratch_shapes=[pltpu.VMEM((FRAME, FRAME), F32), pltpu.SemaphoreType.DMA],
        compiler_params=PARAMS,
        name="roll_step",
    )(positions, owner, which.reshape(1), illumination, intensities)


def sum_kernel(meta, parts, out, acc):
    core, base = meta[128], meta[129]
    acc[...] = jnp.zeros(acc.shape, F32)
    at0 = lax.broadcasted_iota(jnp.int32, (8, 128), 0)
    at1 = lax.broadcasted_iota(jnp.int32, (8, 128), 1)
    column = base + at0
    row = [natural(256 * c + 128 * core + at1) for c in range(2)]

    def step(k, _):
        top, edge = meta[k] >> 9, meta[k] & (FRAME - 1)
        right = column < meta[64 + k]
        for c in range(2):
            below = row[c] < edge
            for plane in range(4):
                g = parts[k, c, plane].astype(F32)
                for tile, piece in ((top, jnp.where(below, 0.0, g)), (top + 1, jnp.where(below, g, 0.0))):
                    acc[0, tile, plane, c] += jnp.where(right, 0.0, piece)
                    acc[1, tile, plane, c] += jnp.where(right, piece, 0.0)
        return 0

    lax.fori_loop(0, 64, step, 0, unroll=4)
    for h in range(2):
        for tile in range(4):
            for plane in range(4):
                for c in range(2):
                    out[4 * h + tile, plane, :, 128 * c : 128 * c + 128] = acc[h, tile, plane, c].astype(BF)


def sum_step(meta, parts):
    return pl.pallas_call(
        sum_kernel,
        out_shape=pltpu.VMEM((8, 4, 8, 256), BF),
        in_specs=[SM, VM],
        out_specs=VM,
        scratch_shapes=[pltpu.VMEM((2, 5, 4, 2, 8, 128), F32)],
        compiler_params=PARAMS,
        name="sum_step",
    )(meta, placed(parts))


def body(transmission, illumination, intensities, scan_positions, tile_owner):
    (far_re, far_im), (prop_re, prop_im) = build_tables()
    half, col = lax.axis_index("half"), lax.axis_index("col")
    which, core = lax.axis_index("zl"), lax.axis_index("core")
    my_col = half * 16 + col
    order = jnp.arange(FRAME, dtype=jnp.int32)
    residue = natural(order)

    place = (residue[None, :] == order[:, None]).astype(BF)
    block = placed(transmission.transpose(0, 1, 3, 2).reshape(128, 512))
    sent = prepare_step(scan_positions, tile_owner, block)
    got = lax.all_to_all(sent.reshape(128, 8, 128), ALL, 0, 0, tiled=True)

    wave, measured = roll_step(scan_positions, tile_owner, which, illumination, intensities)
    tables = (
        right_form(prop_re, prop_im),
        right_form(prop_re, -prop_im),
        right_form(far_re, far_im),
        right_form(far_re.T, -far_im.T),
    )
    got, wave, measured = lax.optimization_barrier((got, wave, measured))

    told = got[::4, 4, :8].astype(jnp.int32).reshape(64, 4)
    rows0 = told[:, 0] * 32 + told[:, 1]
    cols0 = told[:, 2] * 32 + told[:, 3]
    cand = got[:, :4].reshape(2, 2, 8, 4, 4, 128).transpose(0, 3, 1, 4, 2, 5)
    column = (jnp.arange(16, dtype=jnp.int32) * 32 + my_col).reshape(2, 8)
    row = natural((2 * core + which) * 128 + jnp.arange(128, dtype=jnp.int32))
    side = (column[None] < cols0[:, None, None]).astype(jnp.int32)
    tile = rows0[:, None] // 512 + (row[None, :] < rows0[:, None] % 512)
    pick = tile[:, None, None, :] + 4 * side[..., None]
    sent = jnp.zeros((64, 2, 4, 8, 128), BF)
    for a in range(2):
        for b in range(4):
            sent = jnp.where((pick == 4 * a + b)[:, :, None], cand[a, b][None], sent)
    own = lax.all_to_all(sent.reshape(128, 4, 8, 128), ALL, 0, 0, tiled=True).reshape(32, 2, 2, 4, 8, 128)
    other = lax.ppermute(own, "core", [(0, 1), (1, 0)])

    grad, loss = probe_step(core, own, other, wave, measured, tables)

    home = lax.all_to_all(grad.reshape(128, 4, 8, 128), ALL, 0, 0, tiled=True)
    base = col * 32 + (half * 2 + which) * 8
    sums = sum_step(jnp.concatenate([rows0, cols0, jnp.stack([core, base])]), home.reshape(64, 2, 4, 8, 128))
    final = lax.all_to_all(sums, SHARERS, 0, 0, tiled=True)
    final = final.reshape(2, 2, 2, 4, 8, 2, 128).transpose(3, 0, 1, 4, 5, 2, 6).reshape(4, 32, 512)
    gradient = lax.dot_general(place, final, (((1,), (2,)), ((), ())), preferred_element_type=F32)
    gradient = gradient.transpose(1, 0, 2).reshape(2, 2, 512, 32)

    loss = loss[0, :1]
    loss_other = lax.ppermute(loss, "zl", [(0, 1), (1, 0)])
    pair = jnp.concatenate([loss, loss_other])
    probe_losses = jnp.where(which == 0, pair, pair[::-1])
    return gradient, probe_losses


def solution(mesh):
    split = Mesh(mesh.devices.reshape(2, 16, 2, 2), ALL)
    tile = ("zl", "core")
    return jax.shard_map(
        body,
        mesh=split,
        in_specs=(
            P(None, None, tile, PROBE),
            P(),
            P(PROBE, None, None),
            P(PROBE, None),
            P(PROBE),
        ),
        out_specs=(P(None, None, tile, PROBE), P(PROBE)),
        check_vma=False,
    )
```

```python
import math

import jax
import jax.numpy as jnp
import numpy as np
from jax import lax
from jax.experimental import pallas as pl
from jax.experimental.pallas import tpu as pltpu
from jax.sharding import Mesh
from jax.sharding import PartitionSpec as P

FRAME = 512
BORDER = 128
TILE_ROWS = 512
FRESNEL = 0.25
PROBE = ("half", "col")
CHIPS = ("half", "col", "zl")
ALL = ("half", "col", "zl", "core")
SHARERS = ("half", "zl", "core")
BF = jnp.bfloat16
F32 = jnp.float32


def natural(order):
    return order % 16 * 32 + order // 16


def build_tables():
    n = FRAME
    index = np.arange(n)
    angle = (np.float32(-2.0 * math.pi) * (np.outer(index, index) % n).astype(np.float32) / np.float32(n)).astype(np.float32)
    norm = np.float32(1.0 / math.sqrt(n))
    wave_re, wave_im = np.cos(angle) * norm, np.sin(angle) * norm
    freq = np.where(index < n // 2, index, index - n).astype(np.float32)
    phase = (np.float32(-math.pi * FRESNEL) * freq * freq / np.float32(n)).astype(np.float32)
    kre, kim = np.cos(phase)[:, None], np.sin(phase)[:, None]
    sre, sim = kre * wave_re - kim * wave_im, kre * wave_im + kim * wave_re
    prop_re = wave_re @ sre + wave_im @ sim
    prop_im = wave_re @ sim - wave_im @ sre
    perm = natural(index)
    bf = jnp.bfloat16
    far = (wave_re[perm].astype(bf), wave_im[perm].astype(bf))
    prop = (prop_re[perm][:, perm].astype(bf), prop_im[perm][:, perm].astype(bf))
    return far, prop


def right_form(re, im):
    re, im = jnp.asarray(re), jnp.asarray(im)
    return jnp.concatenate([jnp.concatenate([re, im], 1), jnp.concatenate([-im, re], 1)], 0)


def dot(left, right, dims):
    return lax.dot_general(left, right, (dims, ((), ())), preferred_element_type=F32)


NN = ((1,), (0,))
NT = ((1,), (1,))


def probe_kernel(
    core_ref, own, other, wave, bq, measured_hbm, aq_hbm, bw_hbm, aw_hbm, out, loss,
    y, inner, x1, field, turn, measured, aq, bw, aw, sems,
):
    copies = [
        pltpu.make_async_copy(src, dst, sems.at[n])
        for n, (src, dst) in enumerate(
            ((aq_hbm, aq), (bw_hbm, bw), (aw_hbm, aw), (measured_hbm, measured))
        )
    ]
    copies[0].start()
    core = core_ref[0]
    first = core == 0
    here = pl.multiple_of(core * 256, 256)

    def layer(i, z, c, plane):
        mine, rest = own[i, z, c, plane].astype(F32), other[i, z, c, plane].astype(F32)
        return jnp.concatenate([jnp.where(first, mine, rest), jnp.where(first, rest, mine)], axis=0)

    def block_rows(i):
        return pl.ds(pl.multiple_of(i * 16, 16), 16), pl.ds(pl.multiple_of(512 + i * 16, 16), 16)

    def product(plane, get, conj):
        def step(i):
            rows, _ = block_rows(i)
            for z in range(2):
                for c in range(2):
                    at = 256 * c + 128 * z
                    ore, oim = layer(i, z, c, plane), layer(i, z, c, plane + 1)
                    vre, vim = get(i, slice(at, at + 128))
                    if conj:
                        re, im = ore * vre + oim * vim, ore * vim - oim * vre
                    else:
                        re, im = ore * vre - oim * vim, ore * vim + oim * vre
                    y[rows, at : at + 128] = re.astype(BF)
                    y[rows, 512 + at : 640 + at] = im.astype(BF)
            return 0

        for i in range(32):
            step(i)

    def from_wave(i, lanes):
        rows, _ = block_rows(i)
        return wave[0, rows, lanes].astype(F32), wave[1, rows, lanes].astype(F32)

    def from_ref(ref):
        def get(i, lanes):
            rows, rows_im = block_rows(i)
            return ref[rows, lanes], ref[rows_im, lanes]

        return get

    def right(table):
        for n in range(4):
            got = jnp.dot(y[...], table[:, n * 256 : n * 256 + 256], preferred_element_type=F32)
            inner[n // 2 * 512 : n // 2 * 512 + 512, n % 2 * 256 : n % 2 * 256 + 256] = got.astype(BF)

    def left(table, dst):
        for n in range(4):
            rows = slice(n * 256, n * 256 + 256)
            dst[rows, :] = jnp.dot(table[rows, :], inner[...], preferred_element_type=F32)

    def hand_out(plane):
        for o in range(4):
            for j in range(16):
                for part in range(2):
                    rows = pl.ds(part * 512 + 128 * o + j, 8, stride=16)
                    for z in range(2):
                        out[o // 2, j, o % 2, z, plane + part] = turn[z, rows, :].astype(BF)

    product(0, from_wave, False)
    right(bq)
    copies[0].wait()
    for copy in copies[1:]:
        copy.start()
    left(aq, x1)
    product(2, from_ref(x1), False)
    copies[1].wait()
    right(bw)
    copies[2].wait()
    left(aw, field)
    copies[3].wait()

    def compare(i, total):
        rows, rows_im = block_rows(i)
        re, im = field[rows, :], field[rows_im, :]
        misfit = re * re + im * im - measured[rows, :]
        y[rows, 0:512] = (misfit * re).astype(BF)
        y[rows, 512:1024] = (misfit * im).astype(BF)
        return total + misfit * misfit

    total = lax.fori_loop(0, 32, compare, jnp.zeros((16, 512), F32))
    loss[...] = jnp.full((8, 128), jnp.sum(total) * (1.0 / (FRAME * FRAME)), F32)
    right(aw)
    left(bw, field)
    product(2, from_ref(field), True)

    def gradient1(i, _):
        rows, rows_im = block_rows(i)
        for z in range(2):
            lanes = pl.ds(pl.multiple_of(here + z * 128, 128), 128)
            bre, bim = field[rows, lanes], field[rows_im, lanes]
            xre, xim = x1[rows, lanes], x1[rows_im, lanes]
            turn[z, rows, :] = xre * bre + xim * bim
            turn[z, rows_im, :] = xre * bim - xim * bre
        return 0

    lax.fori_loop(0, 32, gradient1, 0, unroll=2)
    hand_out(2)
    for part in range(2):
        cols = pl.ds(pl.multiple_of(here + part * 512, 256), 256)
        got = jnp.dot(y[...], aq[:, cols], preferred_element_type=F32)
        inner[part * 512 : part * 512 + 512, 0:256] = got.astype(BF)
    for n in range(4):
        rows = slice(n * 256, n * 256 + 256)
        field[rows, 0:256] = jnp.dot(bq[rows, :], inner[:, 0:256], preferred_element_type=F32)

    def gradient0(i, _):
        rows, rows_im = block_rows(i)
        for z in range(2):
            bre, bim = field[rows, z * 128 : z * 128 + 128], field[rows_im, z * 128 : z * 128 + 128]
            xre, xim = from_wave(i, pl.ds(pl.multiple_of(here + z * 128, 128), 128))
            turn[z, rows, :] = xre * bre + xim * bim
            turn[z, rows_im, :] = xre * bim - xim * bre
        return 0

    lax.fori_loop(0, 32, gradient0, 0, unroll=2)
    hand_out(0)


VM = pl.BlockSpec(memory_space=pltpu.VMEM)
SM = pl.BlockSpec(memory_space=pltpu.SMEM)
ANY = pl.BlockSpec(memory_space=pl.ANY)
PARAMS = pltpu.CompilerParams(vmem_limit_bytes=56 * 2**20)


def placed(value):
    return pltpu.with_memory_space_constraint(value, pltpu.VMEM)


def probe_step(core, own, other, wave, measured, tables):
    return pl.pallas_call(
        probe_kernel,
        out_shape=(
            pltpu.VMEM((2, 16, 2, 2, 4, 8, 128), BF),
            jax.ShapeDtypeStruct((8, 128), F32),
        ),
        in_specs=[SM] + [VM] * 4 + [ANY] * 4,
        out_specs=(VM, VM),
        scratch_shapes=[
            pltpu.VMEM((512, 1024), BF),
            pltpu.VMEM((1024, 512), BF),
            pltpu.VMEM((1024, 512), F32),
            pltpu.VMEM((1024, 512), F32),
            pltpu.VMEM((2, 1024, 128), F32),
            pltpu.VMEM((512, 512), F32),
        ]
        + [pltpu.VMEM((1024, 1024), BF)] * 3
        + [pltpu.SemaphoreType.DMA((4,))],
        compiler_params=PARAMS,
        name="probe_step",
    )(core.reshape(1), placed(own), placed(other), placed(wave), placed(tables[0]), measured, *tables[1:])


def corner(positions, owner, k):
    return owner[k] * TILE_ROWS - BORDER + positions[k, 0], positions[k, 1]


def prepare_kernel(positions, owner, block, out, rows):
    at0 = lax.broadcasted_iota(jnp.int32, (FRAME, FRAME), 0)
    at1 = lax.broadcasted_iota(jnp.int32, (FRAME, FRAME), 1)
    place = jnp.where(natural(at1) == at0, 1.0, 0.0).astype(BF)
    got = jnp.dot(block[...], place, preferred_element_type=F32)
    lane = lax.broadcasted_iota(jnp.int32, (128, 128), 1)
    info = jnp.zeros((128, 128), jnp.int32)
    for k in range(2):
        for n, value in enumerate(corner(positions, owner, k)):
            info = jnp.where(lane == 4 * k + 2 * n, value >> 5, info)
            info = jnp.where(lane == 4 * k + 2 * n + 1, value & 31, info)
    for q in range(4):
        rows[q, 0:128] = got[:, q * 128 : q * 128 + 128]
        rows[q, 128:256] = info.astype(F32)
    for i in range(32):
        for q in range(4):
            out[i, q % 2, q // 2] = rows[q, pl.ds(i, 8, stride=32), :].astype(BF)


def prepare_step(positions, owner, block):
    return pl.pallas_call(
        prepare_kernel,
        out_shape=pltpu.VMEM((32, 2, 2, 8, 128), BF),
        in_specs=[SM, SM, VM],
        out_specs=VM,
        scratch_shapes=[pltpu.VMEM((4, 256, 128), F32)],
        compiler_params=PARAMS,
        name="prepare_step",
    )(positions, owner, block)


def roll_kernel(positions, owner, which, illumination, intensities, wave, measured, raw, sem):
    copy = pltpu.make_async_copy(intensities.at[which[0]], raw, sem)
    copy.start()
    row0, col0 = corner(positions, owner, which[0])
    at0 = lax.broadcasted_iota(jnp.int32, (FRAME, FRAME), 0)
    at1 = lax.broadcasted_iota(jnp.int32, (FRAME, FRAME), 1)
    cols = jnp.where(((natural(at0) - col0) & (FRAME - 1)) == at1, 1.0, 0.0).astype(BF)
    rows = jnp.where(((natural(at1) - row0) & (FRAME - 1)) == at0, 1.0, 0.0).astype(BF)
    for part in range(2):
        turned = lax.dot_general(cols, illumination[part], (NT, ((), ())), preferred_element_type=F32)
        wave[part] = jnp.dot(turned.astype(BF), rows, preferred_element_type=F32).astype(BF)
    copy.wait()
    measured[...] = raw[...].T


def roll_step(positions, owner, which, illumination, intensities):
    return pl.pallas_call(
        roll_kernel,
        out_shape=(
            pltpu.VMEM((2, FRAME, FRAME), BF),
            jax.ShapeDtypeStruct((FRAME, FRAME), F32),
        ),
        in_specs=[SM, SM, SM, VM, ANY],
        out_specs=(VM, VM),
        scratch_shapes=[pltpu.VMEM((FRAME, FRAME), F32), pltpu.SemaphoreType.DMA],
        compiler_params=PARAMS,
        name="roll_step",
    )(positions, owner, which.reshape(1), illumination, intensities)


def sum_kernel(meta, parts, out, acc):
    core, base = meta[128], meta[129]
    acc[...] = jnp.zeros(acc.shape, F32)
    at0 = lax.broadcasted_iota(jnp.int32, (8, 128), 0)
    at1 = lax.broadcasted_iota(jnp.int32, (8, 128), 1)
    column = base + at0
    row = [natural(256 * c + 128 * core + at1) for c in range(2)]

    def step(k, _):
        top, edge = meta[k] >> 9, meta[k] & (FRAME - 1)
        right = column < meta[64 + k]
        for c in range(2):
            below = row[c] < edge
            for plane in range(4):
                g = parts[k, c, plane].astype(F32)
                for tile, piece in ((top, jnp.where(below, 0.0, g)), (top + 1, jnp.where(below, g, 0.0))):
                    acc[0, tile, plane, c] += jnp.where(right, 0.0, piece)
                    acc[1, tile, plane, c] += jnp.where(right, piece, 0.0)
        return 0

    lax.fori_loop(0, 64, step, 0, unroll=8)
    for h in range(2):
        for tile in range(4):
            for plane in range(4):
                for c in range(2):
                    out[4 * h + tile, plane, :, 128 * c : 128 * c + 128] = acc[h, tile, plane, c].astype(BF)


def sum_step(meta, parts):
    return pl.pallas_call(
        sum_kernel,
        out_shape=pltpu.VMEM((8, 4, 8, 256), BF),
        in_specs=[SM, VM],
        out_specs=VM,
        scratch_shapes=[pltpu.VMEM((2, 5, 4, 2, 8, 128), F32)],
        compiler_params=PARAMS,
        name="sum_step",
    )(meta, placed(parts))


def body(transmission, illumination, intensities, scan_positions, tile_owner):
    (far_re, far_im), (prop_re, prop_im) = build_tables()
    half, col = lax.axis_index("half"), lax.axis_index("col")
    which, core = lax.axis_index("zl"), lax.axis_index("core")
    my_col = half * 16 + col
    order = jnp.arange(FRAME, dtype=jnp.int32)
    residue = natural(order)

    place = (residue[None, :] == order[:, None]).astype(BF)
    block = placed(transmission.transpose(0, 1, 3, 2).reshape(128, 512))
    sent = prepare_step(scan_positions, tile_owner, block)
    got = lax.all_to_all(sent.reshape(128, 8, 128), ALL, 0, 0, tiled=True)

    wave, measured = roll_step(scan_positions, tile_owner, which, illumination, intensities)
    tables = (
        right_form(prop_re, prop_im),
        right_form(prop_re, -prop_im),
        right_form(far_re, far_im),
        right_form(far_re.T, -far_im.T),
    )
    got, wave, measured = lax.optimization_barrier((got, wave, measured))

    told = got[::4, 4, :8].astype(jnp.int32).reshape(64, 4)
    rows0 = told[:, 0] * 32 + told[:, 1]
    cols0 = told[:, 2] * 32 + told[:, 3]
    cand = got[:, :4].reshape(2, 2, 8, 4, 4, 128).transpose(0, 3, 1, 4, 2, 5)
    column = (jnp.arange(16, dtype=jnp.int32) * 32 + my_col).reshape(2, 8)
    row = natural((2 * core + which) * 128 + jnp.arange(128, dtype=jnp.int32))
    side = (column[None] < cols0[:, None, None]).astype(jnp.int32)
    tile = rows0[:, None] // 512 + (row[None, :] < rows0[:, None] % 512)
    pick = tile[:, None, None, :] + 4 * side[..., None]
    sent = jnp.zeros((64, 2, 4, 8, 128), BF)
    for a in range(2):
        for b in range(4):
            sent = jnp.where((pick == 4 * a + b)[:, :, None], cand[a, b][None], sent)
    own = lax.all_to_all(sent.reshape(128, 4, 8, 128), ALL, 0, 0, tiled=True).reshape(32, 2, 2, 4, 8, 128)
    other = lax.ppermute(own, "core", [(0, 1), (1, 0)])

    grad, loss = probe_step(core, own, other, wave, measured, tables)

    home = lax.all_to_all(grad.reshape(128, 4, 8, 128), ALL, 0, 0, tiled=True)
    base = col * 32 + (half * 2 + which) * 8
    sums = sum_step(jnp.concatenate([rows0, cols0, jnp.stack([core, base])]), home.reshape(64, 2, 4, 8, 128))
    final = lax.all_to_all(sums, SHARERS, 0, 0, tiled=True)
    final = final.reshape(2, 2, 2, 4, 8, 2, 128).transpose(3, 0, 1, 4, 5, 2, 6).reshape(4, 32, 512)
    gradient = lax.dot_general(place, final, (((1,), (2,)), ((), ())), preferred_element_type=F32)
    gradient = gradient.transpose(1, 0, 2).reshape(2, 2, 512, 32)

    loss = loss[0, :1]
    loss_other = lax.ppermute(loss, "zl", [(0, 1), (1, 0)])
    pair = jnp.concatenate([loss, loss_other])
    probe_losses = jnp.where(which == 0, pair, pair[::-1])
    return gradient, probe_losses


def solution(mesh):
    split = Mesh(mesh.devices.reshape(2, 16, 2, 2), ALL)
    tile = ("zl", "core")
    return jax.shard_map(
        body,
        mesh=split,
        in_specs=(
            P(None, None, tile, PROBE),
            P(),
            P(PROBE, None, None),
            P(PROBE, None),
            P(PROBE),
        ),
        out_specs=(P(None, None, tile, PROBE), P(PROBE)),
        check_vma=False,
    )
```
